16 devices in a mesh: dp: 1, tp: 16 (over x, y, z, core).
Axes of the slice: x: 2, y: 2, z: 2, core: 2. Of those that a mesh axis runs over, the one named last changes fastest.
Arguments:
- x: bfloat16 [4096, 4608], P(('dp', 'tp'))
- w_gate: bfloat16 [4608, 36864], P(None, 'tp')
- w_up: bfloat16 [4608, 36864], P(None, 'tp')
- w_down: bfloat16 [36864, 4608], P('tp')
Outputs:
- output: bfloat16 [4096, 4608], P(('dp', 'tp'))
All inputs are finite; a program needn't handle non-finite values.
Results may differ from the reference program's by a relative error of at most 0.016.
Values are sent between devices in bfloat16 or wider.
A program may use at most 2 GiB of HBM per device.

```python
import jax
import jax.numpy as jnp

ROWS = 4096
D = 4608
FF = 36864


def setup_inputs(seed: int = 0, part: int = 0) -> dict:
    kx, kg, ku, kd = jax.random.split(jax.random.key(seed), 4)
    drawn = {
        "x": jax.random.normal(jax.random.fold_in(kx, part), (ROWS, D), jnp.float32),
        "w_gate": jax.random.normal(kg, (D, FF), jnp.float32) * D**-0.5,
        "w_up": jax.random.normal(ku, (D, FF), jnp.float32) * D**-0.5,
        "w_down": jax.random.normal(kd, (FF, D), jnp.float32) * FF**-0.5,
    }
    return {k: v.astype(jnp.bfloat16) for k, v in drawn.items()}


def reference(x, w_gate, w_up, w_down):
    gate = jnp.dot(x, w_gate, preferred_element_type=jnp.float32)
    up = jnp.dot(x, w_up, preferred_element_type=jnp.float32)
    hidden = (jax.nn.gelu(gate) * up).astype(jnp.bfloat16)
    return jnp.dot(hidden, w_down, preferred_element_type=jnp.float32).astype(jnp.bfloat16)
```

```python
import functools

import jax
import jax.numpy as jnp
from jax import lax
from jax.experimental import pallas as pl
from jax.experimental.pallas import tpu as pltpu
from jax.sharding import PartitionSpec as P

EXPLICIT = False
MESH = pl.DeviceIdType.MESH
F32, BF16 = jnp.float32, jnp.bfloat16

ROWS = 256
D = 4608
F = 2304
KA, KB = D // 256, F // 256
T9 = 9
CH = D // 2
PARTS = ((0, 96), (96, 80), (176, 80))
SLOTS = 6
PIECE = 64
NP = ROWS // PIECE
LS = 12
ZERO = 63
LAST = 216


def _gelu_mul(g, u):
    t = jnp.tanh(0.7978845608028654 * (g + 0.044715 * (g * g * g)))
    return (g * (0.5 * (1.0 + t)) * u).astype(BF16)


def _kernel(
    x, wg, wu, wd, y, xall,
    xbuf, hid, ring, accbuf, d2s, d2r, ls, recv, emu,
    w_sem, x_sem, ag_send, ag_recv, ad_send, ad_recv, ds_sem, dr_sem, ls_sem, rs_recv,
    *accs,
):
    me = lax.axis_index("tp")
    core = lax.rem(me, 2)
    partner = me + 1 - 2 * core
    axes = [me + m * (1 - 2 * lax.rem(me // m, 2)) for m in (8, 4, 2)]
    nbr = [
        [jnp.where(core == 0, axes[(p + r) % 3], axes[(p + r + 1) % 3]) for r in range(3)]
        for p in range(3)
    ]
    acc = [
        [[accs[(q * 2 + h) * NP + r] for r in range(NP)] for h in range(2)] for q in range(2)
    ] if EXPLICIT else None

    def unit_start(p):
        s = lax.rem(p, SLOTS)
        v = lax.rem(p + 18, 27)
        early = p < 36
        gate_up = early | ((v >= 9) & (p < 198))
        i = jnp.where(early, lax.rem(p, 18), v - 9)
        j = jnp.where(v < 9, v, v - 9)

        @pl.when(gate_up)
        def _():
            cols = pl.ds(pl.multiple_of((i // 2) * 256, 256), 256)
            rows = pl.ds(pl.multiple_of(lax.rem(i, 2) * F, F), F)
            pltpu.make_async_copy(wg.at[rows, cols], ring.at[s, 0], w_sem.at[s, 0]).start()
            pltpu.make_async_copy(wu.at[rows, cols], ring.at[s, 1], w_sem.at[s, 1]).start()

        @pl.when(jnp.logical_not(gate_up) & (p < LAST))
        def _():
            for q in range(2):
                cols = pl.ds(pl.multiple_of(j * 512 + q * 256, 256), 256)
                pltpu.make_async_copy(wd.at[:, cols], ring.at[s, q], w_sem.at[s, q]).start()

    def unit_wait(p):
        s = lax.rem(p, SLOTS)
        for q in range(2):
            pltpu.make_async_copy(wd.at[:, pl.ds(0, 256)], ring.at[s, q], w_sem.at[s, q]).wait()

    def pop(q, h, r):
        if EXPLICIT:
            return pltpu.matmul_pop(acc[q][h][r])
        return emu[q, h, pl.ds(r * PIECE, PIECE), :]

    def half(h, lhs, depth, rhs, after, hooks):
        if not EXPLICIT:
            for k in sorted(hooks):
                hooks[k]()
            for q in range(2):
                tot = None
                for k in range(depth):
                    t = jnp.dot(lhs(h * ROWS, ROWS, k), rhs(q, k), preferred_element_type=F32)
                    tot = t if tot is None else tot + t
                emu[q, h] = tot
            return
        for k in range(depth):
            reg = (h * depth + k) % 2
            for r in range(NP):
                for q in range(2):
                    pltpu.matmul_acc_lhs(
                        acc[q][h][r],
                        lhs(h * ROWS + r * PIECE, PIECE, k),
                        load_staged_rhs=reg if r == 0 else None,
                    )
            for q in range(2):
                w = rhs(q, k + 1) if k + 1 < depth else after(q)
                pltpu.matmul_push_rhs(w, staging_register=1 - reg, mxu_index=q)
            if k in hooks:
                hooks[k]()

    def pop_hidden(h, hb, row0, j):
        cols = pl.ds(pl.multiple_of(j * 256, 256), 256)
        for r in range(NP):
            g, u = pop(0, h, r), pop(1, h, r)
            rows = pl.ds(pl.multiple_of(row0 + r * PIECE, PIECE), PIECE)
            hid[hb, rows, cols] = _gelu_mul(g, u)

    def pop_other(j):
        s = lax.rem(j, 3)
        for r in range(NP):
            for q in range(2):
                d2s[s, pl.ds(r * PIECE, PIECE), pl.ds(q * 256, 256)] = pop(q, 0, r).astype(BF16)

    def pop_own(j):
        for r in range(NP):
            for q in range(2):
                accbuf[j, pl.ds(r * PIECE, PIECE), pl.ds(q * 256, 256)] = pop(q, 1, r)

    def step_a(p, xs, first, second, mid=None, extra=None):
        s = [lax.rem(p + i, SLOTS) for i in range(3)]

        def lhs(row, n, k):
            return xbuf[xs, pl.ds(row, n), pl.ds(k * 256, 256)]

        def rhs(q, k):
            return ring[s[0] if k < 9 else s[1], q, pl.ds((k % 9) * 256, 256), :]

        half(0, lhs, KA, rhs, lambda q: rhs(q, 0), {1: first, **(extra or {})})
        if mid is not None:
            mid()
        half(1, lhs, KA, rhs, lambda q: ring[s[2], q, pl.ds(0, 256), :], {1: second})

    def step_b(p, hb, j, first, extra=None):
        s = [lax.rem(p + i, SLOTS) for i in range(2)]

        def lhs(row, n, k):
            return hid[hb, pl.ds(row, n), pl.ds(k * 256, 256)]

        def rhs(q, k):
            return ring[s[0], q, pl.ds(k * 256, 256), :]

        half(0, lhs, KB, rhs, lambda q: rhs(q, 0), {1: first, **(extra or {})})
        half(1, lhs, KB, rhs, lambda q: ring[s[1], q, pl.ds(0, 256), :], {1: lambda: pop_other(j)})

    def ag_start(src, dst, role, c):
        cols = pl.ds(c * CH, CH)
        for p, (o, n) in enumerate(PARTS):
            rows = pl.ds(o, n)
            pltpu.make_async_remote_copy(
                src_ref=x.at[rows, cols] if src == 0 else xall.at[src - 1, 0, rows, cols],
                dst_ref=xall.at[dst - 1, 0, rows, cols],
                send_sem=ag_send.at[dst - 1, c],
                recv_sem=ag_recv.at[dst - 1, c],
                device_id={"tp": nbr[p][role]},
                device_id_type=MESH,
            ).start()

    def ag_arrived(n, c):
        blk = xall.at[n - 1, 0, :, pl.ds(c * CH, CH)]
        pltpu.make_async_copy(blk, blk, ag_recv.at[n - 1, c]).wait()

    def pass_on(n, c):
        cols = pl.ds(c * CH, CH)
        dst = {0: xbuf.at[0, pl.ds(ROWS, ROWS), cols], 1: xbuf.at[1, pl.ds(0, ROWS), cols]}
        return pltpu.make_async_remote_copy(
            src_ref=x.at[:, cols] if n == 0 else xall.at[n - 1, 0, :, cols],
            dst_ref=dst[n] if n < 2 else xall.at[n - 1, 1, :, cols],
            send_sem=ad_send.at[n, c],
            recv_sem=ad_recv.at[n, c],
            device_id={"tp": partner},
            device_id_type=MESH,
        )

    def passed(n, c):
        blk = x.at[:, pl.ds(0, CH)]
        pltpu.make_async_copy(blk, blk, ad_recv.at[n, c]).wait()

    def x_load(n):
        xs = lax.rem(n, 2)
        return [
            pltpu.make_async_copy(
                xall.at[n - 1, 1 - h], xbuf.at[xs, pl.ds(h * ROWS, ROWS)], x_sem.at[h]
            )
            for h in range(2)
        ]

    def own_load(c):
        cols = pl.ds(c * CH, CH)
        return pltpu.make_async_copy(
            xall.at[0, 0, :, cols], xbuf.at[1, pl.ds(ROWS, ROWS), cols], x_sem.at[c]
        )

    def d2_start(n, j):
        s = lax.rem(j, 3)
        pltpu.make_async_remote_copy(
            src_ref=d2s.at[s],
            dst_ref=d2r.at[lax.rem(n, 2), j],
            send_sem=ds_sem.at[s],
            recv_sem=dr_sem.at[lax.rem(n, 2), j],
            device_id={"tp": partner},
            device_id_type=MESH,
        ).start()

    def d2_sent(j):
        s = lax.rem(j, 3)
        pltpu.make_async_copy(d2s.at[s], d2s.at[s], ds_sem.at[s]).wait()

    def d2_arrived(n, j):
        blk = d2r.at[lax.rem(n, 2), j]
        pltpu.make_async_copy(blk, blk, dr_sem.at[lax.rem(n, 2), j]).wait()

    def sum_start(n, j):
        s = lax.rem(9 * (n - 1) + j, LS)
        for p, (o, rows) in enumerate(PARTS):
            to = jnp.where(n <= 4, nbr[p][0], jnp.where(n <= 6, nbr[p][1], nbr[p][2]))
            pltpu.make_async_remote_copy(
                src_ref=ls.at[s, pl.ds(o, rows)],
                dst_ref=recv.at[9 * (n - 1) + j, pl.ds(o, rows)],
                send_sem=ls_sem.at[s],
                recv_sem=rs_recv.at[n - 1, j],
                device_id={"tp": to},
                device_id_type=MESH,
            ).start()

    def out_start(j):
        s = lax.rem(63 + j, LS)
        cols = pl.ds(pl.multiple_of(j * 512, 512), 512)
        pltpu.make_async_copy(ls.at[s], y.at[:, cols], ls_sem.at[s]).start()

    def sum_sent(g):
        s = lax.rem(g, LS)
        pltpu.make_async_copy(ls.at[s], ls.at[s], ls_sem.at[s]).wait()

    def rs_arrived(n, j):
        blk = recv.at[0]
        pltpu.make_async_copy(blk, blk, rs_recv.at[n - 1, j]).wait()

    def add(n, j, pages, lo, rows=32):
        s = lax.rem(9 * (n - 1) + j, LS)
        sl = pl.ds(lo, rows)
        v = accbuf[j, sl, :] + d2r[lax.rem(n, 2), j, sl, :].astype(F32)
        for g in pages:
            v = v + recv[g, sl, :].astype(F32)
        ls[s, sl, :] = v.astype(BF16)

    def adds(n, j, pages, ks):
        rows = ROWS // len(ks)
        return {
            k: functools.partial(add, n, j, pages, i * rows, rows) for i, k in enumerate(ks)
        }

    def late_pages(n, j):
        return (
            jnp.where(n == 7, 18, 0) + j,
            jnp.where(n == 7, 45, 36) + j,
            jnp.where(n == 7, ZERO, 54 + j),
        )

    def late_arrived(n, j):
        d2_arrived(n, j)

        @pl.when(n == 7)
        def _():
            rs_arrived(3, j)
            rs_arrived(6, j)

        @pl.when(n == 8)
        def _():
            rs_arrived(1, j)
            rs_arrived(5, j)
            rs_arrived(7, j)

    if EXPLICIT:
        for q in range(2):
            for h in range(2):
                for r in range(NP):
                    pop(q, h, r)
    else:
        emu[...] = jnp.zeros_like(emu)
    own = pltpu.make_async_copy(x, xbuf.at[0, pl.ds(0, ROWS)], x_sem.at[0])
    own.start()
    for p in range(SLOTS - 1):
        unit_start(jnp.int32(p))
    barrier = pltpu.get_barrier_semaphore()
    for d in (*axes, partner):
        pl.semaphore_signal(barrier, inc=1, device_id={"tp": d}, device_id_type=MESH)
    pl.semaphore_wait(barrier, 4)
    for c in range(2):
        pass_on(0, c).start()
    for c in range(2):
        ag_start(0, 1, 0, c)
    recv[ZERO] = jnp.zeros_like(recv[ZERO])
    own.wait()
    unit_wait(jnp.int32(0))
    if EXPLICIT:
        for q in range(2):
            pltpu.matmul_push_rhs(ring[0, q, pl.ds(0, 256), :], staging_register=0, mxu_index=q)

    def early(t, _):
        p = 2 * t
        n, j = t // 9, lax.rem(t, 9)
        before = lax.rem(t + 17, 18)
        unit_wait(p + 1)
        unit_wait(p + 2)

        @pl.when(t > 0)
        def _():
            unit_start(p + 4)

        unit_start(p + 5)

        @pl.when(t == 5)
        def _():
            ag_arrived(1, 0)
            pass_on(1, 0).start()
            own_load(0).start()
            ag_start(1, 2, 1, 0)

        @pl.when(t == 8)
        def _():
            ag_arrived(1, 1)
            pass_on(1, 1).start()
            own_load(1).start()
            ag_start(1, 2, 1, 1)
            ag_start(1, 3, 2, 0)
            ag_start(1, 3, 2, 1)

        @pl.when(t == 9)
        def _():
            for c in range(2):
                passed(1, c)
                own_load(c).wait()

        @pl.when(t == 12)
        def _():
            ag_arrived(2, 0)
            pass_on(2, 0).start()
            ag_start(2, 4, 2, 0)

        @pl.when(t == 16)
        def _():
            ag_arrived(2, 1)
            pass_on(2, 1).start()
            ag_start(2, 4, 2, 1)

        def mid():
            @pl.when(t == 0)
            def _():
                passed(0, 0)
                passed(0, 1)

        step_a(
            p,
            n,
            lambda: pop_hidden(
                1, before // 9, jnp.where(before < 9, 0, ROWS), lax.rem(before, 9)
            ),
            lambda: pop_hidden(0, n, jnp.where(n == 0, ROWS, 0), j),
            mid,
        )
        return 0

    lax.fori_loop(0, 18, early, 0)

    def block(n, _):
        base = 36 + 27 * (n - 1)
        unit_wait(base + 1)
        unit_start(base + 4)
        unit_start(base + 5)

        @pl.when(n > 1)
        def _():
            sum_start(n - 1, 8)
            d2_sent(0)

        @pl.when(n < 7)
        def _():
            passed(n + 1, 0)
            passed(n + 1, 1)
            for copy in x_load(n + 1):
                copy.start()

        @pl.when(n == 1)
        def _():
            ag_start(0, 5, 1, 0)
            ag_start(0, 5, 1, 1)

        @pl.when(n == 2)
        def _():
            for c in range(2):
                ag_arrived(4, c)
                pass_on(4, c).start()

        @pl.when(n == 3)
        def _():
            ag_start(0, 7, 2, 0)
            ag_start(0, 7, 2, 1)

        @pl.when(n == 4)
        def _():
            for c in range(2):
                ag_arrived(6, c)
                pass_on(6, c).start()

        @pl.when(n == 5)
        def _():
            for c in range(2):
                ag_arrived(7, c)
                pass_on(7, c).start()

        step_b(base, 1, 0, lambda: pop_hidden(1, 1, ROWS, 8))

        def down(j, _):
            p = base + j
            unit_wait(p + 1)
            unit_start(p + 5)
            d2_start(n, j - 1)

            @pl.when((n > 1) | (j >= 3))
            def _():
                d2_sent(j)

            step_b(p, 1, j, lambda: pop_own(j - 1))
            return 0

        lax.fori_loop(1, jnp.where(n == 7, 3, 9), down, 0)

        @pl.when(n < 7)
        def _():
            mark = base + 9

            def ready(j):
                @pl.when(9 * (n - 1) + j >= LS)
                def _():
                    sum_sent(9 * (n - 1) + j)

                d2_arrived(n, j)

                @pl.when(n == 5)
                def _():
                    rs_arrived(2, j)

                @pl.when(n == 6)
                def _():
                    rs_arrived(4, j)

            def page(j):
                return (jnp.where(n == 5, 9 + j, jnp.where(n == 6, 27 + j, ZERO)),)

            xs = lax.rem(n + 1, 2)
            ks = (3, 5, 7, 9, 11, 13, 15, 16)
            unit_wait(mark + 1)
            unit_wait(mark + 2)
            unit_start(mark + 5)
            d2_start(n, 8)
            for copy in x_load(n + 1):
                copy.wait()

            @pl.when(n == 1)
            def _():
                for c in range(2):
                    ag_arrived(3, c)
                    pass_on(3, c).start()

            @pl.when(n == 2)
            def _():
                for c in range(2):
                    ag_arrived(5, c)
                    pass_on(5, c).start()
                    ag_start(5, 6, 2, c)

            ready(0)
            step_a(
                mark, xs, lambda: pop_own(8), lambda: pop_hidden(0, 1, 0, 0),
                extra=adds(n, 0, page(0), ks),
            )

            def gate_up(j, _):
                p = mark + 2 * j
                unit_wait(p + 1)
                unit_wait(p + 2)
                unit_start(p + 4)
                unit_start(p + 5)
                sum_start(n, j - 1)
                ready(j)
                step_a(
                    p, xs, lambda: pop_hidden(1, 1, ROWS, j - 1), lambda: pop_hidden(0, 1, 0, j),
                    extra=adds(n, j, page(j), ks),
                )
                return 0

            lax.fori_loop(1, 9, gate_up, 0)

        return 0

    lax.fori_loop(1, 8, block, 0)

    def out_or_on(i):
        @pl.when(i < 9)
        def _():
            sum_start(7, i)

        @pl.when(i >= 9)
        def _():
            out_start(i - 9)

    def late(t, _):
        p = 198 + t

        @pl.when(t < 17)
        def _():
            unit_wait(p + 1)

        unit_start(p + 5)
        d2_start(7 + (t - 1) // 9, lax.rem(t - 1, 9))
        d2_sent(lax.rem(t, 9))

        @pl.when(t > 3)
        def _():
            out_or_on(t - 4)

        i = t - 3
        n, j = 7 + i // 9, lax.rem(i, 9)
        sum_sent(54 + i)
        late_arrived(n, j)
        step_b(
            p, jnp.where(t < 9, 1, 0), lax.rem(t, 9), lambda: pop_own(lax.rem(t - 1, 9)),
            extra=adds(n, j, late_pages(n, j), (2, 3, 4, 5, 6, 7, 8)[:4]),
        )
        return 0

    lax.fori_loop(3, 18, late, 0)

    d2_start(jnp.int32(8), jnp.int32(8))
    out_or_on(jnp.int32(14))
    if EXPLICIT:
        for q in range(2):
            pltpu.matmul_acc_lhs(acc[q][0][0], xbuf[0, pl.ds(0, PIECE), pl.ds(0, 256)], load_staged_rhs=0)
            pop(q, 0, 0)
    pop_own(8)
    for j in (6, 7, 8):
        sum_sent(jnp.int32(63 + j))
        late_arrived(jnp.int32(8), jnp.int32(j))
        for lo in range(0, ROWS, 32):
            add(jnp.int32(8), jnp.int32(j), late_pages(jnp.int32(8), j), lo)
        out_start(jnp.int32(j))

    for g in range(60, 72):
        sum_sent(jnp.int32(g))
    for j in (6, 7, 8):
        d2_sent(jnp.int32(j))
    blk = x.at[:, pl.ds(0, CH)]
    for c in range(2):
        for n in range(8):
            pltpu.make_async_copy(blk, blk, ad_send.at[n, c]).wait()
            if n:
                pltpu.make_async_copy(blk, blk, ag_send.at[n - 1, c]).wait()


def _call(x, wg, wu, wd):
    dma = pltpu.SemaphoreType.DMA
    emu_shape = (2, 2, ROWS, 256) if not EXPLICIT else (1, 1, 8, 128)

    def body(*refs):
        if not EXPLICIT:
            _kernel(*refs)
            return
        specs = [pltpu.ACC(q)((PIECE, 256), F32) for q in range(2) for _ in range(2 * NP)]
        pl.run_scoped(lambda *accs: _kernel(*refs, *accs), *specs)

    return pl.pallas_call(
        body,
        out_shape=(
            jax.ShapeDtypeStruct((ROWS, D), BF16),
            jax.ShapeDtypeStruct((7, 2, ROWS, D), BF16),
        ),
        in_specs=[pl.BlockSpec(memory_space=pltpu.HBM)] * 4,
        out_specs=[pl.BlockSpec(memory_space=pltpu.HBM)] * 2,
        scratch_shapes=[
            pltpu.VMEM((2, 2 * ROWS, D), BF16),
            pltpu.VMEM((2, 2 * ROWS, F), BF16),
            pltpu.VMEM((SLOTS, 2, F, 256), BF16),
            pltpu.VMEM((9, ROWS, 512), F32),
            pltpu.VMEM((3, ROWS, 512), BF16),
            pltpu.VMEM((2, 9, ROWS, 512), BF16),
            pltpu.VMEM((LS, ROWS, 512), BF16),
            pltpu.VMEM((64, ROWS, 512), BF16),
            pltpu.VMEM(emu_shape, F32),
            dma((SLOTS, 2)),
            dma((2,)),
            dma((7, 2)),
            dma((7, 2)),
            dma((8, 2)),
            dma((8, 2)),
            dma((3,)),
            dma((2, 9)),
            dma((LS,)),
            dma((7, 9)),
        ],
        compiler_params=pltpu.CompilerParams(
            collective_id=0, has_side_effects=True, vmem_limit_bytes=67_000_000
        ),
        name="mlp",
    )(x, wg, wu, wd)[0]


def solution(mesh):
    return jax.shard_map(
        _call,
        mesh=mesh,
        in_specs=(P(("dp", "tp"), None), P(None, "tp"), P(None, "tp"), P("tp", None)),
        out_specs=P(("dp", "tp"), None),
        check_vma=False,
    )
```

```python
import functools

import jax
import jax.numpy as jnp
from jax import lax
from jax.experimental import pallas as pl
from jax.experimental.pallas import tpu as pltpu
from jax.sharding import PartitionSpec as P

MESH = pl.DeviceIdType.MESH
F32, BF16 = jnp.float32, jnp.bfloat16

ROWS = 256
D = 4608
F = 2304
T = 256
KA, KB = D // T, F // T
W = 3 * T
V = 6 * T
CH = D // 2
PARTS = ((0, 96), (96, 80), (176, 80))
RING = 4
EARLY = 12
FINAL = 66
CHUNKS = 72
LS = 4
A, B, C = range(3)


def _gelu_mul(g, u):
    t = jnp.tanh(0.7978845608028654 * (g + 0.044715 * (g * g * g)))
    return (g * (0.5 * (1.0 + t)) * u).astype(BF16)


def _kernel(
    x, wg, wu, wd, y, xall, rbuf,
    xbuf, hid, ring, accbuf, d2s, d2r, ls, rsum, rlate,
    w_sem, f_sem, x_sem, r_sem, ag_send, ag_recv, ad_send, ad_recv, ds_sem, dr_sem, ls_sem, rs_recv,
):
    me = lax.axis_index("tp")
    core = lax.rem(me, 2)
    partner = me + 1 - 2 * core
    axes = [me + m * (1 - 2 * lax.rem(me // m, 2)) for m in (8, 4, 2)]
    nbr = [
        [jnp.where(core == 0, axes[(p + r) % 3], axes[(p + r + 1) % 3]) for r in range(3)]
        for p in range(3)
    ]

    def local(src, dst, sem):
        return pltpu.make_async_copy(src, dst, sem)

    def await_bytes(ref, sem):
        pltpu.make_async_copy(ref, ref, sem).wait()

    def remote(src, dst, send, recv, to):
        return pltpu.make_async_remote_copy(
            src_ref=src, dst_ref=dst, send_sem=send, recv_sem=recv,
            device_id={"tp": to}, device_id_type=MESH,
        )

    def chunk_start(p):
        s = lax.rem(p, RING)
        v = lax.rem(p + 6, 9)
        early = p < EARLY
        gate_up = early | ((v > 2) & (p < FINAL))
        i = jnp.where(early, lax.rem(p, 6), v - 3)
        j = jnp.where(v > 2, v - 3, v)

        def start(w):
            cols = pl.ds(pl.multiple_of((i // 2) * W, T), W)
            for d in range(2):
                local(
                    w.at[pl.ds(d * F, F), cols], ring.at[s, :, pl.ds(d * W, W)], w_sem.at[s]
                ).start()

        pl.when(gate_up & (lax.rem(i, 2) == 0))(lambda: start(wg))
        pl.when(gate_up & (lax.rem(i, 2) == 1))(lambda: start(wu))

        @pl.when(jnp.logical_not(gate_up) & (p < CHUNKS))
        def _():
            local(wd.at[:, pl.ds(pl.multiple_of(j * V, T), V)], ring.at[s], w_sem.at[s]).start()

    def chunk_wait(p):
        s = lax.rem(p, RING)
        await_bytes(ring.at[s], w_sem.at[s])

    def product(lhs, rhs, depth):
        total = None
        for k in range(depth):
            t = jnp.dot(lhs(k), rhs(k), preferred_element_type=F32)
            total = t if total is None else total + t
        return total

    def tile_a(p, xs, row, i, hb, hrow, j):
        sl = [lax.rem(p + q, RING) for q in range(2)]

        def lhs(k):
            return xbuf[xs, pl.ds(row, ROWS), pl.ds(k * T, T)]

        def rhs(q):
            def tile(k):
                at = pl.multiple_of((k // KB) * W + i * T, T) if not isinstance(i, int) else (k // KB) * W + i * T
                return ring[sl[q], pl.ds((k % KB) * T, T), pl.ds(at, T)]

            return tile

        g, u = product(lhs, rhs(0), KA), product(lhs, rhs(1), KA)
        hid[hb, pl.ds(hrow, ROWS), pl.ds(pl.multiple_of(j * T, T), T)] = _gelu_mul(g, u)

    def step_a(p, xs, hb, flip, e, extra=None):
        for i in range(3):
            for h in range(2):
                row = h * ROWS
                hrow = pl.multiple_of(jnp.where(flip, ROWS - row, row), ROWS)
                tile_a(p, xs, row, i, hb, hrow, 3 * e + i)
                if extra is not None:
                    extra(2 * i + h)

    def step_b(p, hb, j, slot, extra=None):
        s = lax.rem(p, RING)
        for i in range(6):
            for h in range(2):

                def lhs(k, h=h):
                    return hid[hb, pl.ds(h * ROWS, ROWS), pl.ds(k * T, T)]

                def rhs(k, i=i):
                    return ring[s, pl.ds(k * T, T), pl.ds(i * T, T)]

                v = product(lhs, rhs, KB)
                if h == 0:
                    d2s[slot, :, pl.ds(i * T, T)] = v.astype(BF16)
                else:
                    accbuf[:, pl.ds(pl.multiple_of(j * V + i * T, T), T)] = v
            if extra is not None:
                extra(i)

    def ag_start(src, dst, role, c):
        cols = pl.ds(c * CH, CH)
        for p, (o, n) in enumerate(PARTS):
            rows = pl.ds(o, n)
            remote(
                x.at[rows, cols] if src == 0 else xall.at[src - 1, 0, rows, cols],
                xall.at[dst - 1, 0, rows, cols],
                ag_send.at[dst - 1, c],
                ag_recv.at[dst - 1, c],
                nbr[p][role],
            ).start()

    def ag_arrived(n, c):
        await_bytes(xall.at[n - 1, 0, :, pl.ds(c * CH, CH)], ag_recv.at[n - 1, c])

    def pass_on(n, c):
        cols = pl.ds(c * CH, CH)
        if n < 2:
            dst = xbuf.at[n, pl.ds((1 - n) * ROWS, ROWS), cols]
        else:
            dst = xall.at[n - 1, 1, :, cols]
        src = x.at[:, cols] if n == 0 else xall.at[n - 1, 0, :, cols]
        remote(src, dst, ad_send.at[n, c], ad_recv.at[n, c], partner).start()

    def passed(n, c):
        await_bytes(x.at[:, pl.ds(0, CH)], ad_recv.at[n, c])

    def relay(n):
        for c in range(2):
            ag_arrived(n, c)
            pass_on(n, c)

    def x_load(n):
        xs = lax.rem(n, 2)
        return [
            local(xall.at[n - 1, 1 - h], xbuf.at[xs, pl.ds(h * ROWS, ROWS)], x_sem.at[h])
            for h in range(2)
        ]

    def own_load(c):
        cols = pl.ds(c * CH, CH)
        return local(xall.at[0, 0, :, cols], xbuf.at[1, pl.ds(ROWS, ROWS), cols], x_sem.at[c])

    def cols_of(j):
        return pl.ds(pl.multiple_of(j * V, T), V)

    def d2_start(n, j, slot):
        remote(
            d2s.at[slot],
            d2r.at[lax.rem(n, 2), :, cols_of(j)],
            ds_sem.at[slot],
            dr_sem.at[lax.rem(n, 2), j],
            partner,
        ).start()

    def d2_sent(slot):
        await_bytes(d2s.at[slot], ds_sem.at[slot])

    def d2_arrived(n, j):
        await_bytes(d2s.at[0], dr_sem.at[lax.rem(n, 2), j])

    def sum_start(n, j, role, dst):
        s = lax.rem(3 * (n - 1) + j, LS)
        for p, (o, rows) in enumerate(PARTS):
            to = nbr[p][role] if isinstance(role, int) else jnp.where(role, nbr[p][A], nbr[p][B])
            remote(
                ls.at[s, pl.ds(o, rows)],
                dst.at[pl.ds(o, rows), cols_of(j)],
                ls_sem.at[s],
                rs_recv.at[n - 1, j],
                to,
            ).start()

    def sum_on(n, j):
        pl.when(n < 6)(
            lambda: sum_start(n, j, n < 5, rbuf.at[jnp.where(n < 6, n - 1, 0)])
        )
        pl.when(n == 6)(lambda: sum_start(n, j, B, rlate.at[0]))

    def out_start(j):
        s = lax.rem(21 + j, LS)
        local(ls.at[s], y.at[:, cols_of(j)], ls_sem.at[s]).start()

    def sum_sent(g):
        s = lax.rem(g, LS)
        await_bytes(ls.at[s], ls_sem.at[s])

    def rs_arrived(n, j):
        await_bytes(d2s.at[0], rs_recv.at[n - 1, j])

    def add(n, j, terms, i, rows):
        s = lax.rem(3 * (n - 1) + j, LS)
        sl, cols = pl.ds(i * rows, rows), cols_of(j)
        v = accbuf[sl, cols] + d2r[lax.rem(n, 2), sl, cols].astype(F32)
        for ref, r0 in terms:
            v = v + ref[pl.ds(r0 + i * rows, rows), cols].astype(F32)
        ls[s, sl, :] = v.astype(BF16)

    terms_c = ((xbuf.at[0], 0), (rlate.at[0], 0))
    terms_0 = ((xbuf.at[0], ROWS), (xbuf.at[1], 0), (rlate.at[1], 0))
    late_loads = ((2, xbuf.at[0, pl.ds(0, ROWS)]), (0, xbuf.at[0, pl.ds(ROWS, ROWS)]), (4, xbuf.at[1, pl.ds(0, ROWS)]))

    own = local(x, xbuf.at[0, pl.ds(0, ROWS)], x_sem.at[0])
    own.start()
    for i in range(3):
        for q, w in enumerate((wg, wu)):
            for d in range(2):
                local(
                    w.at[pl.ds(d * F, F), pl.ds(i * T, T)],
                    ring.at[q, :, pl.ds(d * W + i * T, T)],
                    f_sem.at[i],
                ).start()
    for p in range(2, RING):
        chunk_start(jnp.int32(p))
    barrier = pltpu.get_barrier_semaphore()
    for d in (*axes, partner):
        pl.semaphore_signal(barrier, inc=1, device_id={"tp": d}, device_id_type=MESH)
    pl.semaphore_wait(barrier, 4)
    for c in range(2):
        pass_on(0, c)
    for c in range(2):
        ag_start(0, 1, A, c)
    rsum[...] = jnp.zeros_like(rsum)
    own.wait()

    def pieces(e):
        first = e == 0

        @pl.when(jnp.logical_not(first))
        def _():
            for q in range(2):
                chunk_wait(2 * e + q)
                chunk_start(2 * e + q + 2)

        def piece(m, _):
            h, i = m // 3, lax.rem(m, 3)

            @pl.when(first & (h == 0))
            def _():
                await_bytes(ring.at[0, :, pl.ds(0, 4 * T)], f_sem.at[i])

            @pl.when(first & (m == 3))
            def _():
                passed(0, 0)
                passed(0, 1)

            for c in range(2):
                @pl.when(jnp.logical_not(first) & (m == 3 * c))
                def _():
                    ag_arrived(1, c)
                    pass_on(1, c)
                    own_load(c).start()
                    ag_start(1, 2, B, c)
                    if c:
                        ag_start(1, 3, C, 0)
                        ag_start(1, 3, C, 1)

            row = pl.multiple_of(h * ROWS, ROWS)
            hrow = pl.multiple_of(ROWS - h * ROWS, ROWS)
            tile_a(2 * e, 0, row, i, 0, hrow, 3 * e + i)
            return 0

        lax.fori_loop(0, 6, piece, 0)

    def early(e, _):
        p = 2 * e
        chunk_wait(p)
        chunk_wait(p + 1)
        chunk_start(p + 2)
        chunk_start(p + 3)

        @pl.when(e == 3)
        def _():
            for c in range(2):
                passed(1, c)
                own_load(c).wait()

        for c in range(2):
            @pl.when(e == 4 + c)
            def _():
                ag_arrived(2, c)
                pass_on(2, c)
                ag_start(2, 4, C, c)

        n = e // 3
        step_a(p, n, n, n == 0, lax.rem(e, 3))
        return 0

    def opening(g, _):
        pieces(2 * g)
        lax.fori_loop(2 * g + 1, 4 * g + 2, early, 0)
        return 0

    lax.fori_loop(0, 2, opening, 0)

    def block(n, _):
        base = EARLY + 9 * (n - 1)

        def down(j, _):
            p = base + j
            slot = lax.rem(n + j, 2)
            chunk_wait(p)
            pl.when(j == 0)(lambda: chunk_start(p + 2))
            chunk_start(p + 3)

            @pl.when(j > 0)
            def _():
                d2_start(n, j - 1, 1 - slot)

            @pl.when((n > 1) | (j > 1))
            def _():
                d2_sent(slot)

            @pl.when(j == 0)
            def _():
                @pl.when(n > 1)
                def _():
                    sum_on(n - 1, 2)

                @pl.when(n < 7)
                def _():
                    passed(n + 1, 0)
                    passed(n + 1, 1)
                    for copy in x_load(n + 1):
                        copy.start()

                @pl.when(n == 1)
                def _():
                    ag_start(0, 5, B, 0)
                    ag_start(0, 5, B, 1)

                @pl.when(n == 3)
                def _():
                    ag_start(0, 7, C, 0)
                    ag_start(0, 7, C, 1)

                for m, blk in ((2, 4), (4, 6), (5, 7)):
                    pl.when(n == m)(functools.partial(relay, blk))

                for m, src in ((5, 2), (6, 4)):
                    @pl.when(n == m)
                    def _():
                        for i in range(3):
                            rs_arrived(src, i)
                        local(rbuf.at[src - 1], rsum, r_sem.at[0]).start()

                @pl.when(n == 7)
                def _():
                    for i, (src, dst) in enumerate(late_loads):
                        for k in range(3):
                            rs_arrived(src + 1, k)
                        local(rbuf.at[src], dst, r_sem.at[i]).start()

            step_b(p, 1, j, slot)
            return 0

        lax.fori_loop(0, jnp.where(n == 7, 1, 3), down, 0)

        def gate_up(j, _):
            p = base + 3 + 2 * j
            chunk_wait(p)
            chunk_wait(p + 1)
            pl.when(j > 0)(lambda: chunk_start(p + 2))
            chunk_start(p + 3)

            @pl.when(j > 0)
            def _():
                sum_on(n, j - 1)

            @pl.when(j == 0)
            def _():
                d2_start(n, 2, lax.rem(n, 2))
                for copy in x_load(n + 1):
                    copy.wait()

                @pl.when(n > 4)
                def _():
                    local(rbuf.at[0], rsum, r_sem.at[0]).wait()

                pl.when(n == 1)(lambda: relay(3))

                @pl.when(n == 2)
                def _():
                    relay(5)
                    for c in range(2):
                        ag_start(5, 6, C, c)

            @pl.when(3 * (n - 1) + j >= LS)
            def _():
                sum_sent(3 * (n - 1) + j)

            d2_arrived(n, j)

            def extra(i):
                if i < 4:
                    add(n, j, ((rsum, 0),), i, ROWS // 4)

            step_a(p, lax.rem(n + 1, 2), 1, False, j, extra)
            return 0

        lax.fori_loop(0, jnp.where(n == 7, 0, 3), gate_up, 0)
        return 0

    lax.fori_loop(1, 8, block, 0)

    def late(n):
        def step(t, _):
            p = FINAL + t
            slot = lax.rem(t + 1, 2)
            chunk_wait(p)
            chunk_start(p + 3)
            d2_start(7 + (t - 1) // 3, lax.rem(t - 1, 3), 1 - slot)
            d2_sent(slot)
            j = lax.rem(t - 1, 3)
            if n == 7:
                pl.when(t > 1)(lambda: sum_start(7, t - 2, C, rlate.at[1]))

                @pl.when(t == 1)
                def _():
                    for i, (src, dst) in enumerate(late_loads):
                        local(rbuf.at[src], dst, r_sem.at[i]).wait()

                rs_arrived(6, j)
            else:
                pl.when(t == 4)(lambda: sum_start(7, 2, C, rlate.at[1]))
                pl.when(t > 4)(lambda: out_start(t - 5))
                rs_arrived(7, j)
            sum_sent(3 * (n - 1) + j)
            d2_arrived(n, j)

            def extra(i):
                if i < 4:
                    add(n, j, terms_c if n == 7 else terms_0, i, ROWS // 4)

            step_b(p, jnp.where(t < 3, 1, 0), lax.rem(t, 3), slot, extra)
            return 0

        return step

    lax.fori_loop(1, 4, late(7), 0)
    lax.fori_loop(4, 6, late(8), 0)

    last = jnp.int32(2)
    d2_start(jnp.int32(8), last, 0)
    out_start(1)
    sum_sent(23)
    d2_arrived(jnp.int32(8), last)
    rs_arrived(7, 2)
    for i in range(8):
        add(jnp.int32(8), 2, terms_0, i, ROWS // 8)
    out_start(2)

    for s in range(LS):
        sum_sent(s)
    d2_sent(0)
    d2_sent(1)
    for c in range(2):
        for n in range(8):
            await_bytes(x.at[:, pl.ds(0, CH)], ad_send.at[n, c])
            if n:
                await_bytes(x.at[:, pl.ds(0, CH)], ag_send.at[n - 1, c])


def _call(x, wg, wu, wd):
    dma = pltpu.SemaphoreType.DMA
    rows = (ROWS, D)
    return pl.pallas_call(
        _kernel,
        out_shape=tuple(
            jax.ShapeDtypeStruct(shape, BF16) for shape in (rows, (7, 2, *rows), (5, *rows))
        ),
        in_specs=[pl.BlockSpec(memory_space=pltpu.HBM)] * 4,
        out_specs=[pl.BlockSpec(memory_space=pltpu.HBM)] * 3,
        scratch_shapes=[
            pltpu.VMEM((2, 2 * ROWS, D), BF16),
            pltpu.VMEM((2, 2 * ROWS, F), BF16),
            pltpu.VMEM((RING, F, V), BF16),
            pltpu.VMEM(rows, F32),
            pltpu.VMEM((2, ROWS, V), BF16),
            pltpu.VMEM((2, *rows), BF16),
            pltpu.VMEM((LS, ROWS, V), BF16),
            pltpu.VMEM(rows, BF16),
            pltpu.VMEM((2, *rows), BF16),
            *(dma(s) for s in ((RING,), (3,), (2,), (3,), (7, 2), (7, 2), (8, 2), (8, 2), (2,), (2, 3), (LS,), (7, 3))),
        ],
        compiler_params=pltpu.CompilerParams(
            collective_id=0, has_side_effects=True, vmem_limit_bytes=67_000_000
        ),
        name="mlp",
    )(x, wg, wu, wd)[0]


def solution(mesh):
    return jax.shard_map(
        _call,
        mesh=mesh,
        in_specs=(P(("dp", "tp"), None), P(None, "tp"), P(None, "tp"), P("tp", None)),
        out_specs=P(("dp", "tp"), None),
        check_vma=False,
    )
```

```python
import functools

import jax
import jax.numpy as jnp
from jax import lax
from jax.experimental import pallas as pl
from jax.experimental.pallas import tpu as pltpu
from jax.sharding import PartitionSpec as P

MESH = pl.DeviceIdType.MESH
F32, BF16 = jnp.float32, jnp.bfloat16

ROWS = 256
D = 4608
F = 2304
T = 256
KA, KB = D // T, F // T
W = 3 * T
V = 6 * T
CH = D // 2
PARTS = ((0, 96), (96, 80), (176, 80))
RING = 4
EARLY = 12
FINAL = 66
LS = 4
A, B, C = range(3)


def _gelu_mul(g, u):
    t = jnp.tanh(0.7978845608028654 * (g + 0.044715 * (g * g * g)))
    return (g * (0.5 * (1.0 + t)) * u).astype(BF16)


def _when(cond):
    def run(f):
        def trip(_, carry):
            f()
            return carry

        lax.fori_loop(0, jnp.where(cond, 1, 0), trip, 0)

    return run


def _kernel(
    x, wg, wu, wd, y, xall, rbuf,
    xbuf, hub, ring, accbuf, d2s, ls, rsum, rlate,
    w_sem, f_sem, x_sem, r_sem, ag_send, ag_recv, ad_send, ad_recv, ds_sem, dr_sem, ls_sem, rs_recv,
):
    me = lax.axis_index("tp")
    core = lax.rem(me, 2)
    partner = me + 1 - 2 * core
    axes = [me + m * (1 - 2 * lax.rem(me // m, 2)) for m in (8, 4, 2)]
    nbr = [
        [jnp.where(core == 0, axes[(p + r) % 3], axes[(p + r + 1) % 3]) for r in range(3)]
        for p in range(3)
    ]

    def local(src, dst, sem):
        return pltpu.make_async_copy(src, dst, sem)

    def await_bytes(ref, sem):
        pltpu.make_async_copy(ref, ref, sem).wait()

    def remote(src, dst, send, recv, to):
        return pltpu.make_async_remote_copy(
            src_ref=src, dst_ref=dst, send_sem=send, recv_sem=recv,
            device_id={"tp": to}, device_id_type=MESH,
        )

    def load_one(w, i, p):
        s = lax.rem(p, RING)
        cols = pl.ds(pl.multiple_of(i * W, T), W)
        for d in range(2):
            local(
                w.at[pl.ds(d * F, F), cols], ring.at[s, :, pl.ds(d * W, W)], w_sem.at[s]
            ).start()

    def load_pair(i, p):
        load_one(wg, i, p)
        load_one(wu, i, p + 1)

    def load_down(j, p):
        s = lax.rem(p, RING)
        local(wd.at[:, pl.ds(j * V, V)], ring.at[s], w_sem.at[s]).start()

    def chunk_wait(p):
        s = lax.rem(p, RING)
        await_bytes(ring.at[s], w_sem.at[s])

    def product(lhs, rhs, depth):
        total = None
        for k in range(depth):
            t = jnp.dot(lhs(k), rhs(k), preferred_element_type=F32)
            total = t if total is None else total + t
        return total

    def tile_a(p, xs, row, i, hb, half, j):
        sl = [lax.rem(p + q, RING) for q in range(2)]

        def lhs(k):
            return xbuf[xs, pl.ds(row, ROWS), pl.ds(k * T, T)]

        def rhs(q):
            def tile(k):
                at = pl.multiple_of((k // KB) * W + i * T, T) if not isinstance(i, int) else (k // KB) * W + i * T
                return ring[sl[q], pl.ds((k % KB) * T, T), pl.ds(at, T)]

            return tile

        g, u = product(lhs, rhs(0), KA), product(lhs, rhs(1), KA)
        hub[hb, :, pl.ds(pl.multiple_of(half * F + j * T, T), T)] = _gelu_mul(g, u)

    def step_a(p, xs, hb, flip, e, extra=None):
        for i in range(3):
            for h in range(2):
                tile_a(p, xs, h * ROWS, i, hb, jnp.where(flip, 1 - h, h), 3 * e + i)
                if extra is not None:
                    extra(2 * i + h)

    def step_b(p, j, slot):
        s = lax.rem(p, RING)
        for i in range(6):
            d2s[slot, :, pl.ds(i * T, T)] = rows_b(1, 0, i, s).astype(BF16)
            accbuf[:, pl.ds(pl.multiple_of(j * V + i * T, T), T)] = rows_b(1, 1, i, s)

    def rows_b(hb, h, i, s):
        def lhs(k):
            return hub[hb, :, pl.ds(h * F + k * T, T)]

        def rhs(k):
            return ring[s, pl.ds(k * T, T), pl.ds(i * T, T)]

        return product(lhs, rhs, KB)

    def ag_start(src, dst, role, c):
        cols = pl.ds(c * CH, CH)
        for p, (o, n) in enumerate(PARTS):
            rows = pl.ds(o, n)
            remote(
                x.at[rows, cols] if src == 0 else xall.at[src - 1, 0, rows, cols],
                xall.at[dst - 1, 0, rows, cols],
                ag_send.at[dst - 1, c],
                ag_recv.at[dst - 1, c],
                nbr[p][role],
            ).start()

    def ag_arrived(n, c):
        await_bytes(xall.at[n - 1, 0, :, pl.ds(c * CH, CH)], ag_recv.at[n - 1, c])

    def pass_on(n, c):
        cols = pl.ds(c * CH, CH)
        if n < 2:
            dst = xbuf.at[n, pl.ds((1 - n) * ROWS, ROWS), cols]
        else:
            dst = xall.at[n - 1, 1, :, cols]
        src = x.at[:, cols] if n == 0 else xall.at[n - 1, 0, :, cols]
        remote(src, dst, ad_send.at[n, c], ad_recv.at[n, c], partner).start()

    def passed(n, c):
        await_bytes(x.at[:, pl.ds(0, CH)], ad_recv.at[n, c])

    def relay(n):
        for c in range(2):
            ag_arrived(n, c)
            pass_on(n, c)

    def x_load(n):
        xs = lax.rem(n, 2)
        return [
            local(xall.at[n - 1, 1 - h], xbuf.at[xs, pl.ds(h * ROWS, ROWS)], x_sem.at[h])
            for h in range(2)
        ]

    def own_load(c):
        cols = pl.ds(c * CH, CH)
        return local(xall.at[0, 0, :, cols], xbuf.at[1, pl.ds(ROWS, ROWS), cols], x_sem.at[c])

    def cols_of(j):
        return pl.ds(pl.multiple_of(j * V, T), V)

    def d2_start(n, j, slot):
        remote(
            d2s.at[slot],
            hub.at[2 + lax.rem(n, 2), :, cols_of(j)],
            ds_sem.at[slot],
            dr_sem.at[lax.rem(n, 2), j],
            partner,
        ).start()

    def d2_sent(slot):
        await_bytes(d2s.at[slot], ds_sem.at[slot])

    def d2_arrived(n, j):
        await_bytes(d2s.at[0], dr_sem.at[lax.rem(n, 2), j])

    def sum_start(n, j, role, dst):
        s = lax.rem(3 * (n - 1) + j, LS)
        for p, (o, rows) in enumerate(PARTS):
            to = nbr[p][C] if role is None else jnp.where(role, nbr[p][A], nbr[p][B])
            remote(
                ls.at[s, pl.ds(o, rows)],
                dst.at[pl.ds(o, rows), cols_of(j)],
                ls_sem.at[s],
                rs_recv.at[n - 1, j],
                to,
            ).start()

    def sum_on(n, j):
        sum_start(n, j, n < 5, rbuf.at[n - 1])

    def out_start(j):
        s = lax.rem(21 + j, LS)
        local(ls.at[s], y.at[:, cols_of(j)], ls_sem.at[s]).start()

    def sum_sent(g):
        s = lax.rem(g, LS)
        await_bytes(ls.at[s], ls_sem.at[s])

    def rs_arrived(n, j):
        await_bytes(d2s.at[0], rs_recv.at[n - 1, j])

    def term(n, cols, terms, v):
        v = v + hub[2 + lax.rem(n, 2), :, cols].astype(F32)
        for ref, r0 in terms:
            v = v + ref[pl.ds(r0, ROWS), cols].astype(F32)
        return v.astype(BF16)

    def add(n, j, terms, i):
        s = lax.rem(3 * (n - 1) + j, LS)
        cols = pl.ds(pl.multiple_of(j * V + i * T, T), T)
        ls[s, :, pl.ds(i * T, T)] = term(n, cols, terms, accbuf[:, cols])

    terms_c = ((xbuf.at[0], 0), (xbuf.at[1], ROWS))
    terms_0 = ((xbuf.at[0], ROWS), (xbuf.at[1], 0), (rlate, 0))

    def r_load(i, src, dst, col=0, width=D):
        cols = pl.ds(col, width)
        h, r = dst
        return local(rbuf.at[src - 1, :, cols], xbuf.at[h, pl.ds(r, ROWS), cols], r_sem.at[i])

    late_loads = (
        r_load(0, 3, (0, 0)), r_load(1, 6, (1, ROWS), 0, 2 * V), r_load(2, 6, (1, ROWS), 2 * V, V),
        r_load(3, 1, (0, ROWS)), r_load(4, 5, (1, 0)),
    )

    own = local(x, xbuf.at[0, pl.ds(0, ROWS)], x_sem.at[0])
    own.start()
    for i in range(3):
        for q, w in enumerate((wg, wu)):
            for d in range(2):
                local(
                    w.at[pl.ds(d * F, F), pl.ds(i * T, T)],
                    ring.at[q, :, pl.ds(d * W + i * T, T)],
                    f_sem.at[i],
                ).start()
    load_pair(1, 2)
    barrier = pltpu.get_barrier_semaphore()
    for d in (*axes, partner):
        pl.semaphore_signal(barrier, inc=1, device_id={"tp": d}, device_id_type=MESH)
    pl.semaphore_wait(barrier, 4)
    for c in range(2):
        pass_on(0, c)
    for c in range(2):
        ag_start(0, 1, A, c)
    rsum[...] = jnp.zeros_like(rsum)
    own.wait()

    def pieces(e):
        first = e == 0

        @_when(jnp.logical_not(first))
        def _():
            for q in range(2):
                chunk_wait(4 + q)
            load_pair(0, 6)

        def piece(m, _):
            h, i = m // 3, lax.rem(m, 3)

            @pl.when(first & (h == 0))
            def _():
                await_bytes(ring.at[0, :, pl.ds(0, 4 * T)], f_sem.at[i])

            @pl.when(first & (m == 3))
            def _():
                passed(0, 0)
                passed(0, 1)

            @_when(jnp.logical_not(first) & (i == 0))
            def _():
                for c in range(2):
                    @_when(m == 3 * c)
                    def _():
                        ag_arrived(1, c)
                        pass_on(1, c)
                        own_load(c).start()
                        ag_start(1, 2, B, c)
                        if c:
                            ag_start(1, 3, C, 0)
                            ag_start(1, 3, C, 1)

            tile_a(2 * e, 0, pl.multiple_of(h * ROWS, ROWS), i, 0, 1 - h, 3 * e + i)
            return 0

        lax.fori_loop(0, 6, piece, 0)

    def early(e, _):
        p = 2 * e
        chunk_wait(p)
        chunk_wait(p + 1)

        @_when(e < 5)
        def _():
            load_pair(lax.rem(e + 1, 3), p + 2)

        @_when(e >= 3)
        def _():
            @_when(e == 3)
            def _():
                for c in range(2):
                    passed(1, c)
                    own_load(c).wait()

            for c in range(2):
                @_when(e == 4 + c)
                def _():
                    ag_arrived(2, c)
                    pass_on(2, c)
                    ag_start(2, 4, C, c)
                    if c:
                        load_down(0, EARLY)
                        load_down(1, EARLY + 1)

        n = e // 3
        step_a(p, n, n, n == 0, lax.rem(e, 3))
        return 0

    def opening(g, _):
        pieces(2 * g)
        lax.fori_loop(2 * g + 1, 4 * g + 2, early, 0)
        return 0

    lax.fori_loop(0, 2, opening, 0)

    def block(n, _):
        base = EARLY + 9 * (n - 1)

        def down(j, _):
            p = base + j
            slot = lax.rem(n + j, 2)
            chunk_wait(p)

            @_when(j > 0)
            def _():
                d2_start(n, j - 1, 1 - slot)
                pl.when(j == 1)(lambda: load_one(wu, 0, p + 3))
                pl.when(j == 2)(lambda: load_one(wg, 1, p + 3))

            @pl.when((n > 1) | (j > 1))
            def _():
                d2_sent(slot)

            @_when(j == 0)
            def _():
                load_down(2, p + 2)
                load_one(wg, 0, p + 3)

                @_when(n > 1)
                def _():
                    sum_on(n - 1, 2)

                passed(n + 1, 0)
                passed(n + 1, 1)
                for copy in x_load(n + 1):
                    copy.start()

                for m, role in ((1, B), (3, C)):
                    @_when(n == m)
                    def _():
                        for c in range(2):
                            ag_start(0, m + 4, role, c)

                for m, blk in ((2, 4), (4, 6), (5, 7)):
                    _when(n == m)(functools.partial(relay, blk))

                for m, src in ((5, 2), (6, 4)):
                    @_when(n == m)
                    def _():
                        for i in range(3):
                            rs_arrived(src, i)
                        local(rbuf.at[src - 1], rsum, r_sem.at[0]).start()

            step_b(p, j, slot)
            return 0

        lax.fori_loop(0, 3, down, 0)

        def gate_up(j, _):
            p = base + 3 + 2 * j
            chunk_wait(p)
            chunk_wait(p + 1)

            @_when(j == 0)
            def _():
                d2_start(n, 2, lax.rem(n, 2))
                load_one(wu, 1, p + 3)
                for copy in x_load(n + 1):
                    copy.wait()

                @pl.when(n > 4)
                def _():
                    local(rbuf.at[0], rsum, r_sem.at[0]).wait()

                _when(n == 1)(lambda: relay(3))

                @_when(n == 2)
                def _():
                    relay(5)
                    for c in range(2):
                        ag_start(5, 6, C, c)

            @_when(j > 0)
            def _():
                sum_on(n, j - 1)
                _when(j == 1)(lambda: load_pair(2, p + 2))

                @_when(j == 2)
                def _():
                    for i in range(2):
                        load_down(i, p + 2 + i)

            @pl.when(3 * (n - 1) + j >= LS)
            def _():
                sum_sent(3 * (n - 1) + j)

            d2_arrived(n, j)

            def extra(i):
                for t in ((0, 1), (2,), (3,), (4,), (5,), ())[i]:
                    add(n, j, ((rsum, 0),), t)

            step_a(p, lax.rem(n + 1, 2), 1, False, j, extra)
            return 0

        lax.fori_loop(0, 3, gate_up, 0)
        return 0

    lax.fori_loop(1, 7, block, 0)

    def group(s, g, hb, h, store):
        for i in range(6):
            store(i, rows_b(hb, h, i, s))

    def on_c(j):
        sum_start(7, j, None, rlate)

    tops = (
        lambda: (sum_on(6, 2), load_down(2, FINAL + 2), chunk_wait(FINAL), d2_sent(0), d2_sent(1),
                 [rs_arrived(n, k) for n in (1, 3, 5) for k in range(3)], rs_arrived(6, 0), rs_arrived(6, 1),
                 [late_loads[i].start() for i in (0, 1, 3, 4)]),
        lambda: (d2_start(7, 0, 0), chunk_wait(FINAL + 1)),
        lambda: (d2_start(7, 1, 1), late_loads[0].wait(), late_loads[1].wait(), d2_arrived(7, 0), sum_sent(18)),
        lambda: (on_c(0), chunk_wait(FINAL + 2), d2_sent(0)),
        lambda: (d2_start(7, 2, 0), d2_arrived(7, 1), sum_sent(19), rs_arrived(6, 2), late_loads[2].start()),
        lambda: (on_c(1), d2_sent(1)),
        lambda: (d2_start(8, 0, 1), d2_arrived(7, 2), sum_sent(20), late_loads[2].wait()),
        lambda: (on_c(2), d2_sent(0)),
        lambda: (d2_start(8, 1, 0), d2_sent(1)),
        lambda: (d2_start(8, 2, 1), d2_arrived(8, 0), rs_arrived(7, 0), sum_sent(21), late_loads[3].wait(), late_loads[4].wait()),
        lambda: (out_start(0), d2_arrived(8, 1), rs_arrived(7, 1), sum_sent(22)),
    )

    def late(t, _):
        for lo, hi in ((0, 4), (4, 8), (8, 11)):
            @_when((t >= lo) & (t < hi))
            def _():
                for i in range(lo, hi):
                    _when(t == i)(tops[i])

        w_c = (t == 2) | (t == 4) | (t == 6)
        w_0 = t > 8
        o = jnp.where(t < 2, t, jnp.where(t == 3, 2, jnp.where(t == 5, 3, t - 3)))
        g = jnp.where(w_c, t // 2 - 1, jnp.where(w_0, t - 9, lax.rem(o, 3)))
        s = lax.rem(FINAL + g, RING)

        @pl.when(jnp.logical_not(w_c | w_0))
        def _():
            def store(i, v):
                d2s[lax.rem(o, 2), :, pl.ds(i * T, T)] = v.astype(BF16)

            group(s, g, jnp.where(o < 3, 1, 0), 0, store)

        for cond, n, terms in ((w_c, 7, terms_c), (w_0, 8, terms_0)):
            @pl.when(cond)
            def _():
                def store(i, v):
                    cols = pl.ds(pl.multiple_of(g * V + i * T, T), T)
                    ls[lax.rem(3 * (n - 1) + g, LS), :, pl.ds(i * T, T)] = term(n, cols, terms, v)

                group(s, g, 8 - n, 1, store)

        return 0

    lax.fori_loop(0, 11, late, 0)

    last = 2
    out_start(1)
    sum_sent(23)
    d2_arrived(8, last)

    def keep(i, v):
        cols = pl.ds(last * V + i * T, T)
        accbuf[:, cols] = v

    group((FINAL + last) % RING, last, 0, 1, keep)
    rs_arrived(7, last)
    for i in range(6):
        add(8, last, terms_0, i)
    out_start(last)

    for s in range(LS):
        sum_sent(s)
    d2_sent(0)
    d2_sent(1)
    for c in range(2):
        for n in range(8):
            await_bytes(x.at[:, pl.ds(0, CH)], ad_send.at[n, c])
            if n:
                await_bytes(x.at[:, pl.ds(0, CH)], ag_send.at[n - 1, c])


def _call(x, wg, wu, wd):
    dma = pltpu.SemaphoreType.DMA
    rows = (ROWS, D)
    return pl.pallas_call(
        _kernel,
        out_shape=tuple(
            jax.ShapeDtypeStruct(shape, BF16) for shape in (rows, (7, 2, *rows), (6, *rows))
        ),
        in_specs=[pl.BlockSpec(memory_space=pltpu.HBM)] * 4,
        out_specs=[pl.BlockSpec(memory_space=pltpu.HBM)] * 3,
        scratch_shapes=[
            pltpu.VMEM((2, 2 * ROWS, D), BF16),
            pltpu.VMEM((4, *rows), BF16),
            pltpu.VMEM((RING, F, V), BF16),
            pltpu.VMEM(rows, F32),
            pltpu.VMEM((2, ROWS, V), BF16),
            pltpu.VMEM((LS, ROWS, V), BF16),
            pltpu.VMEM(rows, BF16),
            pltpu.VMEM(rows, BF16),
            *(dma(s) for s in ((RING,), (3,), (2,), (5,), (7, 2), (7, 2), (8, 2), (8, 2), (2,), (2, 3), (LS,), (7, 3))),
        ],
        compiler_params=pltpu.CompilerParams(
            collective_id=0, has_side_effects=True, vmem_limit_bytes=67_000_000
        ),
        name="mlp",
    )(x, wg, wu, wd)[0]


def solution(mesh):
    return jax.shard_map(
        _call,
        mesh=mesh,
        in_specs=(P(("dp", "tp"), None), P(None, "tp"), P(None, "tp"), P("tp", None)),
        out_specs=P(("dp", "tp"), None),
        check_vma=False,
    )
```

```python
import functools

import jax
import jax.numpy as jnp
from jax import lax
from jax.experimental import pallas as pl
from jax.experimental.pallas import tpu as pltpu
from jax.sharding import PartitionSpec as P

MESH = pl.DeviceIdType.MESH
F32, BF16 = jnp.float32, jnp.bfloat16

ROWS = 256
D = 4608
F = 2304
T = 256
KA, KB = D // T, F // T
W = 3 * T
V = 6 * T
CH = D // 2
PARTS = ((0, 96), (96, 80), (176, 80))
RING = 4
EARLY = 12
FINAL = 66
LS = 4
SLICE = 16
A, B, C = range(3)


def _gelu_mul(g, u):
    t = jnp.tanh(0.7978845608028654 * (g + 0.044715 * (g * g * g)))
    return (g * (0.5 * (1.0 + t)) * u).astype(BF16)


def _when(cond):
    def run(f):
        def trip(_, carry):
            f()
            return carry

        lax.fori_loop(0, jnp.where(cond, 1, 0), trip, 0)

    return run


def _kernel(
    x, wg, wu, wd, y, xall, rbuf,
    xbuf, hub, ring, accbuf, d2s, ls, rsum, rlate,
    w_sem, f_sem, x_sem, r_sem, ag_send, ag_recv, ad_recv, ds_sem, dr_sem, ls_sem, rs_recv,
):
    me = lax.axis_index("tp")
    core = lax.rem(me, 2)
    partner = me + 1 - 2 * core
    axes = [me + m * (1 - 2 * lax.rem(me // m, 2)) for m in (8, 4, 2)]
    nbr = [
        [jnp.where(core == 0, axes[(p + r) % 3], axes[(p + r + 1) % 3]) for r in range(3)]
        for p in range(3)
    ]

    def local(src, dst, sem):
        return pltpu.make_async_copy(src, dst, sem)

    def await_bytes(ref, sem):
        pltpu.make_async_copy(ref, ref, sem).wait()

    def remote(src, dst, send, recv, to):
        return pltpu.make_async_remote_copy(
            src_ref=src, dst_ref=dst, send_sem=send, recv_sem=recv,
            device_id={"tp": to}, device_id_type=MESH,
        )

    def load_one(w, i, p):
        s = lax.rem(p, RING)
        cols = pl.ds(pl.multiple_of(i * W, T), W)
        for d in range(2):
            local(
                w.at[pl.ds(d * F, F), cols], ring.at[s, :, pl.ds(d * W, W)], w_sem.at[s]
            ).start()

    def load_pair(i, p):
        load_one(wg, i, p)
        load_one(wu, i, p + 1)

    def load_down(j, p):
        s = lax.rem(p, RING)
        local(wd.at[:, pl.ds(j * V, V)], ring.at[s], w_sem.at[s]).start()

    def chunk_wait(p):
        s = lax.rem(p, RING)
        await_bytes(ring.at[s], w_sem.at[s])

    def product(lhs, rhs, depth):
        total = None
        for k in range(depth):
            t = jnp.dot(lhs(k), rhs(k), preferred_element_type=F32)
            total = t if total is None else total + t
        return total

    def tile_a(p, xs, row, i, hb, half, j, extra=None):
        sl = [lax.rem(p + q, RING) for q in range(2)]

        def lhs(k):
            return xbuf[xs, pl.ds(row, ROWS), pl.ds(k * T, T)]

        def rhs(q):
            def tile(k):
                at = pl.multiple_of((k // KB) * W + i * T, T) if not isinstance(i, int) else (k // KB) * W + i * T
                return ring[sl[q], pl.ds((k % KB) * T, T), pl.ds(at, T)]

            return tile

        g, u = product(lhs, rhs(0), KA), product(lhs, rhs(1), KA)
        cols = pl.ds(pl.multiple_of(half * F + j * T, T), T)
        if extra is not None:
            extra()
        hub[hb, :, cols] = _gelu_mul(g, u)

    def step_a(p, xs, hb, flip, e, extra=None):
        for i in range(3):
            for h in range(2):
                tile_a(
                    p, xs, h * ROWS, i, hb, jnp.where(flip, 1 - h, h), 3 * e + i,
                    extra and functools.partial(extra, 2 * i + h),
                )

    def step_b(p, j, slot):
        s = lax.rem(p, RING)
        for i in range(6):
            d2s[slot, :, pl.ds(i * T, T)] = rows_b(1, 0, i, s).astype(BF16)
            accbuf[:, pl.ds(pl.multiple_of(j * V + i * T, T), T)] = rows_b(1, 1, i, s)

    def rows_b(hb, h, i, s):
        def lhs(k):
            return hub[hb, :, pl.ds(h * F + k * T, T)]

        def rhs(k):
            return ring[s, pl.ds(k * T, T), pl.ds(i * T, T)]

        return product(lhs, rhs, KB)

    def ag_start(src, dst, role, c):
        cols = pl.ds(c * CH, CH)
        for p, (o, n) in enumerate(PARTS):
            rows = pl.ds(o, n)
            remote(
                x.at[rows, cols] if src == 0 else xall.at[src - 1, 0, rows, cols],
                xall.at[dst - 1, 0, rows, cols],
                ag_send.at[0],
                ag_recv.at[dst - 1, c],
                nbr[p][role],
            ).start()

    def ag_arrived(n, c):
        await_bytes(xall.at[n - 1, 0, :, pl.ds(c * CH, CH)], ag_recv.at[n - 1, c])

    def pass_on(n, c):
        cols = pl.ds(c * CH, CH)
        if n < 2:
            dst = xbuf.at[n, pl.ds((1 - n) * ROWS, ROWS), cols]
        else:
            dst = xall.at[n - 1, 1, :, cols]
        src = x.at[:, cols] if n == 0 else xall.at[n - 1, 0, :, cols]
        remote(src, dst, ag_send.at[1], ad_recv.at[n, c], partner).start()

    def passed(n, c):
        await_bytes(x.at[:, pl.ds(0, CH)], ad_recv.at[n, c])

    def relay(n):
        for c in range(2):
            ag_arrived(n, c)
            pass_on(n, c)

    def x_load(n):
        xs = lax.rem(n, 2)
        return [
            local(xall.at[n - 1, 1 - h], xbuf.at[xs, pl.ds(h * ROWS, ROWS)], x_sem.at[h])
            for h in range(2)
        ]

    def own_load(c):
        cols = pl.ds(c * CH, CH)
        return local(xall.at[0, 0, :, cols], xbuf.at[1, pl.ds(ROWS, ROWS), cols], x_sem.at[c])

    def cols_of(j):
        return pl.ds(pl.multiple_of(j * V, T), V)

    def d2_start(n, j, slot):
        remote(
            d2s.at[slot],
            hub.at[2 + lax.rem(n, 2), :, cols_of(j)],
            ds_sem.at[slot],
            dr_sem.at[lax.rem(n, 2), j],
            partner,
        ).start()

    def d2_sent(slot):
        await_bytes(d2s.at[slot], ds_sem.at[slot])

    def d2_arrived(n, j):
        await_bytes(d2s.at[0], dr_sem.at[lax.rem(n, 2), j])

    def sum_start(n, j, role, dst):
        s = lax.rem(3 * (n - 1) + j, LS)
        for p, (o, rows) in enumerate(PARTS):
            to = nbr[p][C] if role is None else jnp.where(role, nbr[p][A], nbr[p][B])
            remote(
                ls.at[s, pl.ds(o, rows)],
                dst.at[pl.ds(o, rows), cols_of(j)],
                ls_sem.at[s],
                rs_recv.at[n - 1, j],
                to,
            ).start()

    def sum_on(n, j):
        sum_start(n, j, n < 5, rbuf.at[n - 1])

    def out_start(j):
        s = lax.rem(21 + j, LS)
        local(ls.at[s], y.at[:, cols_of(j)], ls_sem.at[s]).start()

    def sum_sent(g):
        s = lax.rem(g, LS)
        await_bytes(ls.at[s], ls_sem.at[s])

    def rs_arrived(n, j):
        await_bytes(d2s.at[0], rs_recv.at[n - 1, j])

    def add(n, j, terms, i, value=None):
        s = lax.rem(3 * (n - 1) + j, LS)
        cols = pl.ds(pl.multiple_of(j * V + i * T, T), T)
        size = SLICE if value is None else ROWS
        for r in range(0, ROWS, size):
            rows = pl.ds(r, size)
            v = accbuf[rows, cols] if value is None else value
            v = v + hub[2 + lax.rem(n, 2), rows, cols].astype(F32)
            for ref, r0 in terms:
                v = v + ref[pl.ds(r0 + r, size), cols].astype(F32)
            ls[s, rows, pl.ds(i * T, T)] = v.astype(BF16)

    terms_c = ((xbuf.at[0], 0), (xbuf.at[1], ROWS))
    terms_0 = ((xbuf.at[0], ROWS), (xbuf.at[1], 0), (rlate, 0))

    def r_load(i, src, dst, col=0, width=D):
        cols = pl.ds(col, width)
        h, r = dst
        return local(rbuf.at[src - 1, :, cols], xbuf.at[h, pl.ds(r, ROWS), cols], r_sem.at[i])

    late_loads = (
        r_load(0, 3, (0, 0)), *(r_load(1 + k, 6, (1, ROWS), k * V, V) for k in range(3)),
        r_load(4, 1, (0, ROWS)), r_load(5, 5, (1, 0)),
    )

    def first_tile(i):
        for q, w in enumerate((wg, wu)):
            for d in range(2):
                local(
                    w.at[pl.ds(d * F, F), pl.ds(i * T, T)],
                    ring.at[q, :, pl.ds(d * W + i * T, T)],
                    f_sem.at[i],
                ).start()

    own = local(x, xbuf.at[0, pl.ds(0, ROWS)], x_sem.at[0])
    own.start()
    first_tile(0)
    barrier = pltpu.get_barrier_semaphore()
    for d in (*axes, partner):
        pl.semaphore_signal(barrier, inc=1, device_id={"tp": d}, device_id_type=MESH)
    rsum[...] = jnp.zeros_like(rsum)
    first_tile(1)
    pl.semaphore_wait(barrier, 4)
    for c in range(2):
        pass_on(0, c)
    for c in range(2):
        ag_start(0, 1, A, c)
    own.wait()

    def piece(i, _):
        await_bytes(ring.at[0, :, pl.ds(0, 4 * T)], f_sem.at[i])
        _when(i == 0)(lambda: first_tile(2))
        _when(i == 1)(lambda: load_pair(1, 2))
        tile_a(0, 0, 0, i, 0, 1, i)
        return 0

    lax.fori_loop(0, 3, piece, 0)

    def third(m, _):
        @_when(m == 0)
        def _():
            passed(0, 0)
            passed(0, 1)

        @_when(m > 0)
        def _():
            @_when(m == 1)
            def _():
                for q in range(2):
                    chunk_wait(4 + q)
                load_pair(0, 6)

            for c in range(2):
                @_when(m == 1 + c)
                def _():
                    ag_arrived(1, c)
                    pass_on(1, c)
                    own_load(c).start()
                    ag_start(1, 2, B, c)
                    if c:
                        ag_start(1, 3, C, 0)
                        ag_start(1, 3, C, 1)

        h = jnp.where(m == 1, 0, 1)
        e = jnp.where(m == 0, 0, 2)
        for i in range(3):
            tile_a(2 * e, 0, pl.multiple_of(h * ROWS, ROWS), i, 0, 1 - h, 3 * e + i)
        return 0

    def third_hop(c):
        ag_arrived(2, c)
        pass_on(2, c)
        ag_start(2, 4, C, c)

    def early(e, _):
        p = 2 * e
        chunk_wait(p)
        chunk_wait(p + 1)

        @_when(e < 5)
        def _():
            load_pair(lax.rem(e + 1, 3), p + 2)

        @_when(e >= 3)
        def _():
            @_when(e == 3)
            def _():
                for c in range(2):
                    passed(1, c)
                    own_load(c).wait()

            _when(e == 4)(lambda: third_hop(0))

            @_when(e == 5)
            def _():
                for i in range(2):
                    load_down(i, EARLY + i)

        n = e // 3
        step_a(p, n, n, n == 0, lax.rem(e, 3))
        return 0

    def opening(g, _):
        lax.fori_loop(g, 2 * g + 1, third, 0)
        lax.fori_loop(2 * g + 1, 4 * g + 2, early, 0)
        return 0

    lax.fori_loop(0, 2, opening, 0)

    def block(n, _):
        base = EARLY + 9 * (n - 1)

        def down(j, _):
            p = base + j
            slot = lax.rem(n + j, 2)
            chunk_wait(p)

            @_when(j > 0)
            def _():
                d2_start(n, j - 1, 1 - slot)
                _when(j == 2)(lambda: load_one(wg, 1, p + 3))

                @_when(j == 1)
                def _():
                    load_one(wu, 0, p + 3)
                    passed(n + 1, 0)
                    passed(n + 1, 1)
                    for copy in x_load(n + 1):
                        copy.start()

            @pl.when((n > 1) | (j > 1))
            def _():
                d2_sent(slot)

            @_when(j == 0)
            def _():
                load_down(2, p + 2)
                load_one(wg, 0, p + 3)

                @_when(n > 1)
                def _():
                    sum_on(n - 1, 2)

                _when(n == 1)(lambda: third_hop(1))

                for m, role in ((1, B), (3, C)):
                    @_when(n == m)
                    def _():
                        for c in range(2):
                            ag_start(0, m + 4, role, c)

                for m, blk in ((2, 4), (4, 6), (5, 7)):
                    _when(n == m)(functools.partial(relay, blk))

                for m, src in ((5, 2), (6, 4)):
                    @_when(n == m)
                    def _():
                        for i in range(3):
                            rs_arrived(src, i)
                        local(rbuf.at[src - 1], rsum, r_sem.at[0]).start()

            step_b(p, j, slot)
            return 0

        lax.fori_loop(0, 3, down, 0)

        def gate_up(j, _):
            p = base + 3 + 2 * j
            chunk_wait(p)
            chunk_wait(p + 1)

            @_when(j == 0)
            def _():
                d2_start(n, 2, lax.rem(n, 2))
                load_one(wu, 1, p + 3)
                for copy in x_load(n + 1):
                    copy.wait()

                @pl.when(n > 4)
                def _():
                    local(rbuf.at[0], rsum, r_sem.at[0]).wait()

                _when(n == 1)(lambda: relay(3))

                @_when(n == 2)
                def _():
                    relay(5)
                    for c in range(2):
                        ag_start(5, 6, C, c)

            @_when(j > 0)
            def _():
                sum_on(n, j - 1)
                _when(j == 1)(lambda: load_pair(2, p + 2))

                @_when(j == 2)
                def _():
                    for i in range(2):
                        load_down(i, p + 2 + i)

            @pl.when(3 * (n - 1) + j >= LS)
            def _():
                sum_sent(3 * (n - 1) + j)

            d2_arrived(n, j)

            def extra(i):
                for t in ((0, 1), (2,), (3,), (4,), (5,), ())[i]:
                    add(n, j, ((rsum, 0),), t)

            step_a(p, lax.rem(n + 1, 2), 1, False, j, extra)
            return 0

        lax.fori_loop(0, 3, gate_up, 0)
        return 0

    lax.fori_loop(1, 7, block, 0)

    def group(s, g, hb, h, store):
        for i in range(6):
            store(i, rows_b(hb, h, i, s))

    def on_c(j):
        sum_start(7, j, None, rlate)

    def r_due(k):
        rs_arrived(6, k)
        late_loads[1 + k].start()

    tops = (
        lambda: (sum_on(6, 2), load_down(2, FINAL + 2), chunk_wait(FINAL), d2_sent(0), d2_sent(1),
                 [rs_arrived(n, k) for n in (1, 3, 5) for k in range(3)], r_due(0),
                 [late_loads[i].start() for i in (0, 4, 5)]),
        lambda: (d2_start(7, 0, 0), chunk_wait(FINAL + 1)),
        lambda: (d2_start(7, 1, 1), late_loads[0].wait(), late_loads[1].wait(), d2_arrived(7, 0), sum_sent(18), r_due(1)),
        lambda: (on_c(0), chunk_wait(FINAL + 2), d2_sent(0)),
        lambda: (d2_start(7, 2, 0), d2_arrived(7, 1), sum_sent(19), late_loads[2].wait()),
        lambda: (on_c(1), d2_sent(1), r_due(2)),
        lambda: (d2_start(8, 0, 1), d2_arrived(7, 2), sum_sent(20), late_loads[3].wait()),
        lambda: d2_sent(0),
        lambda: (d2_start(8, 1, 0), d2_sent(1), on_c(2)),
        lambda: (d2_start(8, 2, 1), d2_arrived(8, 0), rs_arrived(7, 0), sum_sent(21), late_loads[4].wait(), late_loads[5].wait()),
        lambda: (out_start(0), d2_arrived(8, 1), rs_arrived(7, 1), sum_sent(22)),
    )

    def late(t, _):
        for lo, hi in ((0, 4), (4, 8), (8, 11)):
            @_when((t >= lo) & (t < hi))
            def _():
                for i in range(lo, hi):
                    _when(t == i)(tops[i])

        w_c = (t == 2) | (t == 4) | (t == 6)
        w_0 = t > 8
        o = jnp.where(t < 2, t, jnp.where(t == 3, 2, jnp.where(t == 5, 3, t - 3)))
        g = jnp.where(w_c, t // 2 - 1, jnp.where(w_0, t - 9, lax.rem(o, 3)))
        s = lax.rem(FINAL + g, RING)

        @pl.when(jnp.logical_not(w_c | w_0))
        def _():
            def store(i, v):
                d2s[lax.rem(o, 2), :, pl.ds(i * T, T)] = v.astype(BF16)

            group(s, g, jnp.where(o < 3, 1, 0), 0, store)

        for cond, n, terms in ((w_c, 7, terms_c), (w_0, 8, terms_0)):
            @pl.when(cond)
            def _():
                group(s, g, 8 - n, 1, lambda i, v: add(n, g, terms, i, v))

        return 0

    lax.fori_loop(0, 11, late, 0)

    last = 2
    out_start(1)
    sum_sent(23)
    d2_arrived(8, last)

    def keep(i, v):
        cols = pl.ds(last * V + i * T, T)
        accbuf[:, cols] = v

    group((FINAL + last) % RING, last, 0, 1, keep)
    rs_arrived(7, last)
    for half in range(2):
        for i in range(3):
            add(8, last, terms_0, 3 * half + i)
        lo = half * W
        local(
            ls.at[23 % LS, :, pl.ds(lo, W)], y.at[:, pl.ds(last * V + lo, W)], ls_sem.at[23 % LS]
        ).start()

    d2_sent(0)
    d2_sent(1)
    await_bytes(xall.at[:, 0], ag_send.at[0])
    await_bytes(xall.at[pl.ds(0, 4)], ag_send.at[1])
    for s in range(LS):
        sum_sent(s)


def _copy(src, dst, buf, get, put):
    n = get.shape[0]
    step = ROWS // n
    rows = [pl.ds(i * step, step) for i in range(n)]
    gets = [pltpu.make_async_copy(src.at[r], buf.at[r], get.at[i]) for i, r in enumerate(rows)]
    puts = [pltpu.make_async_copy(buf.at[r], dst.at[r], put.at[i]) for i, r in enumerate(rows)]
    for g in gets:
        g.start()
    for g, p in zip(gets, puts):
        g.wait()
        p.start()
    for p in puts:
        p.wait()


def _call(x, wg, wu, wd):
    dma = pltpu.SemaphoreType.DMA
    rows = (ROWS, D)
    out = pl.pallas_call(
        _kernel,
        out_shape=tuple(
            jax.ShapeDtypeStruct(shape, BF16) for shape in (rows, (7, 2, *rows), (6, *rows))
        ),
        in_specs=[pl.BlockSpec(memory_space=pltpu.HBM)] * 4,
        out_specs=[pl.BlockSpec(memory_space=pltpu.HBM)] * 3,
        scratch_shapes=[
            pltpu.VMEM((2, 2 * ROWS, D), BF16),
            pltpu.VMEM((4, *rows), BF16),
            pltpu.VMEM((RING, F, V), BF16),
            pltpu.VMEM(rows, F32),
            pltpu.VMEM((2, ROWS, V), BF16),
            pltpu.VMEM((LS, ROWS, V), BF16),
            pltpu.VMEM(rows, BF16),
            pltpu.VMEM(rows, BF16),
            *(dma(s) for s in ((RING,), (3,), (2,), (6,), (2,), (7, 2), (8, 2), (2,), (2, 3), (LS,), (7, 3))),
        ],
        compiler_params=pltpu.CompilerParams(
            collective_id=0, has_side_effects=True, vmem_limit_bytes=67_000_000
        ),
        name="mlp",
    )(x, wg, wu, wd)[0]
    return pl.pallas_call(
        _copy,
        out_shape=jax.ShapeDtypeStruct(rows, BF16),
        in_specs=[pl.BlockSpec(memory_space=pltpu.HBM)],
        out_specs=pl.BlockSpec(memory_space=pltpu.HBM),
        scratch_shapes=[pltpu.VMEM(rows, BF16), dma((8,)), dma((8,))],
        name="hand_over",
    )(out)


def solution(mesh):
    return jax.shard_map(
        _call,
        mesh=mesh,
        in_specs=(P(("dp", "tp"), None), P(None, "tp"), P(None, "tp"), P("tp", None)),
        out_specs=P(("dp", "tp"), None),
        check_vma=False,
    )
```

```python
import functools

import jax
import jax.numpy as jnp
from jax import lax
from jax.experimental import pallas as pl
from jax.experimental.pallas import tpu as pltpu
from jax.sharding import PartitionSpec as P

MESH = pl.DeviceIdType.MESH
F32, BF16 = jnp.float32, jnp.bfloat16

ROWS = 256
D = 4608
F = 2304
T = 256
KA, KB = D // T, F // T
W = 3 * T
V = 6 * T
CH = D // 2
PARTS = ((0, 96), (96, 80), (176, 80))
RING = 4
EARLY = 12
FINAL = 66
LS = 4
SLICE = 16
A, B, C = range(3)


def _gelu_mul(g, u):
    t = jnp.tanh(0.7978845608028654 * (g + 0.044715 * (g * g * g)))
    return (g * (0.5 * (1.0 + t)) * u).astype(BF16)


def _when(cond):
    def run(f):
        def trip(_, carry):
            f()
            return carry

        lax.fori_loop(0, jnp.where(cond, 1, 0), trip, 0)

    return run


def _kernel(
    x, wg, wu, wd, y, xall, rbuf,
    xbuf, hub, ring, accbuf, d2s, ls, rsum, rlate, pair,
    w_sem, f_sem, x_sem, r_sem, ag_send, ag_recv, ad_recv, ds_sem, dr_sem, ls_sem, rs_recv,
):
    me = lax.axis_index("tp")
    core = lax.rem(me, 2)
    partner = me + 1 - 2 * core
    axes = [me + m * (1 - 2 * lax.rem(me // m, 2)) for m in (8, 4, 2)]
    nbr = [
        [jnp.where(core == 0, axes[(p + r) % 3], axes[(p + r + 1) % 3]) for r in range(3)]
        for p in range(3)
    ]

    def local(src, dst, sem):
        return pltpu.make_async_copy(src, dst, sem)

    def await_bytes(ref, sem):
        pltpu.make_async_copy(ref, ref, sem).wait()

    def remote(src, dst, send, recv, to):
        return pltpu.make_async_remote_copy(
            src_ref=src, dst_ref=dst, send_sem=send, recv_sem=recv,
            device_id={"tp": to}, device_id_type=MESH,
        )

    def load_one(w, i, p):
        s = lax.rem(p, RING)
        cols = pl.ds(pl.multiple_of(i * W, T), W)
        for d in range(2):
            local(
                w.at[pl.ds(d * F, F), cols], ring.at[s, :, pl.ds(d * W, W)], w_sem.at[s]
            ).start()

    def load_pair(i, p):
        load_one(wg, i, p)
        load_one(wu, i, p + 1)

    def load_down(j, p):
        s = lax.rem(p, RING)
        local(wd.at[:, pl.ds(j * V, V)], ring.at[s], w_sem.at[s]).start()

    def chunk_wait(p):
        s = lax.rem(p, RING)
        await_bytes(ring.at[s], w_sem.at[s])

    def product(lhs, rhs, depth):
        total = None
        for k in range(depth):
            t = jnp.dot(lhs(k), rhs(k), preferred_element_type=F32)
            total = t if total is None else total + t
        return total

    def tile_a(p, xs, row, i, hb, half, j, extra=None):
        sl = [lax.rem(p + q, RING) for q in range(2)]

        def lhs(k):
            return xbuf[xs, pl.ds(row, ROWS), pl.ds(k * T, T)]

        def rhs(q):
            def tile(k):
                at = pl.multiple_of((k // KB) * W + i * T, T) if not isinstance(i, int) else (k // KB) * W + i * T
                return ring[sl[q], pl.ds((k % KB) * T, T), pl.ds(at, T)]

            return tile

        g, u = product(lhs, rhs(0), KA), product(lhs, rhs(1), KA)
        cols = pl.ds(pl.multiple_of(half * F + j * T, T), T)
        if extra is None:
            hub[hb, :, cols] = _gelu_mul(g, u)
            return
        pair[0], pair[1] = g, u
        for r in range(0, ROWS, SLICE):
            rows = pl.ds(r, SLICE)
            extra(r)
            hub[hb, rows, cols] = _gelu_mul(pair[0, rows], pair[1, rows])

    def step_a(p, xs, hb, flip, e, extra=None):
        for i in range(3):
            for h in range(2):
                tile_a(
                    p, xs, h * ROWS, i, hb, jnp.where(flip, 1 - h, h), 3 * e + i,
                    extra and functools.partial(extra, 2 * i + h),
                )

    def step_b(p, j, slot):
        s = lax.rem(p, RING)
        for i in range(6):
            d2s[slot, :, pl.ds(i * T, T)] = rows_b(1, 0, i, s).astype(BF16)
            accbuf[:, pl.ds(pl.multiple_of(j * V + i * T, T), T)] = rows_b(1, 1, i, s)

    def rows_b(hb, h, i, s):
        def lhs(k):
            return hub[hb, :, pl.ds(h * F + k * T, T)]

        def rhs(k):
            return ring[s, pl.ds(k * T, T), pl.ds(i * T, T)]

        return product(lhs, rhs, KB)

    def ag_start(src, dst, role, c):
        cols = pl.ds(c * CH, CH)
        for p, (o, n) in enumerate(PARTS):
            rows = pl.ds(o, n)
            remote(
                x.at[rows, cols] if src == 0 else xall.at[src - 1, 0, rows, cols],
                xall.at[dst - 1, 0, rows, cols],
                ag_send.at[0],
                ag_recv.at[dst - 1, c],
                nbr[p][role],
            ).start()

    def ag_arrived(n, c):
        await_bytes(xall.at[n - 1, 0, :, pl.ds(c * CH, CH)], ag_recv.at[n - 1, c])

    def pass_on(n, c):
        cols = pl.ds(c * CH, CH)
        if n < 2:
            dst = xbuf.at[n, pl.ds((1 - n) * ROWS, ROWS), cols]
        else:
            dst = xall.at[n - 1, 1, :, cols]
        src = x.at[:, cols] if n == 0 else xall.at[n - 1, 0, :, cols]
        remote(src, dst, ag_send.at[1], ad_recv.at[n, c], partner).start()

    def passed(n, c):
        await_bytes(x.at[:, pl.ds(0, CH)], ad_recv.at[n, c])

    def relay(n):
        for c in range(2):
            ag_arrived(n, c)
            pass_on(n, c)

    def x_load(n):
        xs = lax.rem(n, 2)
        return [
            local(xall.at[n - 1, 1 - h], xbuf.at[xs, pl.ds(h * ROWS, ROWS)], x_sem.at[h])
            for h in range(2)
        ]

    def own_load(c):
        cols = pl.ds(c * CH, CH)
        return local(xall.at[0, 0, :, cols], xbuf.at[1, pl.ds(ROWS, ROWS), cols], x_sem.at[c])

    def cols_of(j):
        return pl.ds(pl.multiple_of(j * V, T), V)

    def d2_start(n, j, slot):
        remote(
            d2s.at[slot],
            hub.at[2 + lax.rem(n, 2), :, cols_of(j)],
            ds_sem.at[slot],
            dr_sem.at[lax.rem(n, 2), j],
            partner,
        ).start()

    def d2_sent(slot):
        await_bytes(d2s.at[slot], ds_sem.at[slot])

    def d2_arrived(n, j):
        await_bytes(d2s.at[0], dr_sem.at[lax.rem(n, 2), j])

    def sum_start(n, j, role, dst):
        s = lax.rem(3 * (n - 1) + j, LS)
        for p, (o, rows) in enumerate(PARTS):
            to = nbr[p][C] if role is None else jnp.where(role, nbr[p][A], nbr[p][B])
            remote(
                ls.at[s, pl.ds(o, rows)],
                dst.at[pl.ds(o, rows), cols_of(j)],
                ls_sem.at[s],
                rs_recv.at[n - 1, j],
                to,
            ).start()

    def sum_on(n, j):
        sum_start(n, j, n < 5, rbuf.at[n - 1])

    def sum_sent(g):
        s = lax.rem(g, LS)
        await_bytes(ls.at[s], ls_sem.at[s])

    def rs_arrived(n, j):
        await_bytes(d2s.at[0], rs_recv.at[n - 1, j])

    def add_rows(n, j, terms, i, r, value=None):
        size = SLICE if value is None else ROWS
        cols = pl.ds(pl.multiple_of(j * V + i * T, T), T)
        rows = pl.ds(r, size)
        v = accbuf[rows, cols] if value is None else value
        v = v + hub[2 + lax.rem(n, 2), rows, cols].astype(F32)
        for ref, r0 in terms:
            v = v + ref[pl.ds(r0 + r, size), cols].astype(F32)
        if isinstance(n, int) and n == 8:
            y[rows, cols] = v.astype(BF16)
        else:
            ls[lax.rem(3 * (n - 1) + j, LS), rows, pl.ds(i * T, T)] = v.astype(BF16)

    def add(n, j, terms, i, value=None):
        for r in range(0, ROWS, SLICE if value is None else ROWS):
            add_rows(n, j, terms, i, r, value)

    terms_c = ((xbuf.at[0], 0), (xbuf.at[1], ROWS))
    terms_0 = ((xbuf.at[0], ROWS), (xbuf.at[1], 0), (rlate, 0))

    def r_load(i, src, dst, col=0, width=D):
        cols = pl.ds(col, width)
        h, r = dst
        return local(rbuf.at[src - 1, :, cols], xbuf.at[h, pl.ds(r, ROWS), cols], r_sem.at[i])

    late_loads = (
        r_load(0, 3, (0, 0)), *(r_load(1 + k, 6, (1, ROWS), k * V, V) for k in range(3)),
        r_load(4, 1, (0, ROWS)), r_load(5, 5, (1, 0)),
    )

    def first_tile(i):
        for q, w in enumerate((wg, wu)):
            for d in range(2):
                local(
                    w.at[pl.ds(d * F, F), pl.ds(i * T, T)],
                    ring.at[q, :, pl.ds(d * W + i * T, T)],
                    f_sem.at[i],
                ).start()

    own = local(x, xbuf.at[0, pl.ds(0, ROWS)], x_sem.at[0])
    own.start()
    first_tile(0)
    barrier = pltpu.get_barrier_semaphore()
    for d in (*axes, partner):
        pl.semaphore_signal(barrier, inc=1, device_id={"tp": d}, device_id_type=MESH)
    rsum[...] = jnp.zeros_like(rsum)
    first_tile(1)
    pl.semaphore_wait(barrier, 4)
    for c in range(2):
        pass_on(0, c)
    for c in range(2):
        ag_start(0, 1, A, c)
    own.wait()

    def piece(i, _):
        await_bytes(ring.at[0, :, pl.ds(0, 4 * T)], f_sem.at[i])
        _when(i == 0)(lambda: first_tile(2))
        _when(i == 1)(lambda: load_pair(1, 2))
        tile_a(0, 0, 0, i, 0, 1, i)
        return 0

    lax.fori_loop(0, 3, piece, 0)

    def third(m, _):
        @_when(m == 0)
        def _():
            passed(0, 0)
            passed(0, 1)

        @_when(m > 0)
        def _():
            @_when(m == 1)
            def _():
                for q in range(2):
                    chunk_wait(4 + q)
                load_pair(0, 6)

            for c in range(2):
                @_when(m == 1 + c)
                def _():
                    ag_arrived(1, c)
                    pass_on(1, c)
                    own_load(c).start()
                    ag_start(1, 2, B, c)
                    if c:
                        ag_start(1, 3, C, 0)
                        ag_start(1, 3, C, 1)

        h = jnp.where(m == 1, 0, 1)
        e = jnp.where(m == 0, 0, 2)
        for i in range(3):
            tile_a(2 * e, 0, pl.multiple_of(h * ROWS, ROWS), i, 0, 1 - h, 3 * e + i)
        return 0

    def third_hop(c):
        ag_arrived(2, c)
        pass_on(2, c)
        ag_start(2, 4, C, c)

    def early(e, _):
        p = 2 * e
        chunk_wait(p)
        chunk_wait(p + 1)

        @_when(e < 5)
        def _():
            load_pair(lax.rem(e + 1, 3), p + 2)

        @_when(e >= 3)
        def _():
            @_when(e == 3)
            def _():
                for c in range(2):
                    passed(1, c)
                    own_load(c).wait()

            _when(e == 4)(lambda: third_hop(0))

            @_when(e == 5)
            def _():
                for i in range(2):
                    load_down(i, EARLY + i)

        n = e // 3
        step_a(p, n, n, n == 0, lax.rem(e, 3))
        return 0

    def opening(g, _):
        lax.fori_loop(g, 2 * g + 1, third, 0)
        lax.fori_loop(2 * g + 1, 4 * g + 2, early, 0)
        return 0

    lax.fori_loop(0, 2, opening, 0)

    def block(n, _):
        base = EARLY + 9 * (n - 1)

        def down(j, _):
            p = base + j
            slot = lax.rem(n + j, 2)
            chunk_wait(p)

            @_when(j > 0)
            def _():
                d2_start(n, j - 1, 1 - slot)
                _when(j == 2)(lambda: load_one(wg, 1, p + 3))

                @_when(j == 1)
                def _():
                    load_one(wu, 0, p + 3)
                    passed(n + 1, 0)
                    passed(n + 1, 1)
                    for copy in x_load(n + 1):
                        copy.start()

            @pl.when((n > 1) | (j > 1))
            def _():
                d2_sent(slot)

            @_when(j == 0)
            def _():
                load_down(2, p + 2)
                load_one(wg, 0, p + 3)

                @_when(n > 1)
                def _():
                    sum_on(n - 1, 2)

                _when(n == 1)(lambda: third_hop(1))

                for m, role in ((1, B), (3, C)):
                    @_when(n == m)
                    def _():
                        for c in range(2):
                            ag_start(0, m + 4, role, c)

                for m, blk in ((2, 4), (4, 6), (5, 7)):
                    _when(n == m)(functools.partial(relay, blk))

                for m, src in ((5, 2), (6, 4)):
                    @_when(n == m)
                    def _():
                        for i in range(3):
                            rs_arrived(src, i)
                        local(rbuf.at[src - 1], rsum, r_sem.at[0]).start()

            step_b(p, j, slot)
            return 0

        lax.fori_loop(0, 3, down, 0)

        def gate_up(j, _):
            p = base + 3 + 2 * j
            chunk_wait(p)
            chunk_wait(p + 1)

            @_when(j == 0)
            def _():
                d2_start(n, 2, lax.rem(n, 2))
                load_one(wu, 1, p + 3)
                for copy in x_load(n + 1):
                    copy.wait()

                @pl.when(n > 4)
                def _():
                    local(rbuf.at[0], rsum, r_sem.at[0]).wait()

                _when(n == 1)(lambda: relay(3))

                @_when(n == 2)
                def _():
                    relay(5)
                    for c in range(2):
                        ag_start(5, 6, C, c)

            @_when(j > 0)
            def _():
                sum_on(n, j - 1)
                _when(j == 1)(lambda: load_pair(2, p + 2))

                @_when(j == 2)
                def _():
                    for i in range(2):
                        load_down(i, p + 2 + i)

            @pl.when(3 * (n - 1) + j >= LS)
            def _():
                sum_sent(3 * (n - 1) + j)

            d2_arrived(n, j)

            def extra(i, r):
                q = (i * ROWS + r) // SLICE
                for k in range(6 * q // 5, 6 * (q + 1) // 5):
                    t, row = divmod(k * SLICE, ROWS)
                    if t < 6:
                        add_rows(n, j, ((rsum, 0),), t, row)

            step_a(p, lax.rem(n + 1, 2), 1, False, j, extra)
            return 0

        lax.fori_loop(0, 3, gate_up, 0)
        return 0

    lax.fori_loop(1, 7, block, 0)

    def group(s, g, hb, h, store):
        for i in range(6):
            store(i, rows_b(hb, h, i, s))

    def on_c(j):
        sum_start(7, j, None, rlate)

    def r_due(k):
        rs_arrived(6, k)
        late_loads[1 + k].start()

    tops = (
        lambda: (sum_on(6, 2), load_down(2, FINAL + 2), chunk_wait(FINAL), d2_sent(0), d2_sent(1),
                 [rs_arrived(n, k) for n in (1, 3, 5) for k in range(3)], r_due(0),
                 [late_loads[i].start() for i in (0, 4, 5)]),
        lambda: (d2_start(7, 0, 0), chunk_wait(FINAL + 1)),
        lambda: (d2_start(7, 1, 1), late_loads[0].wait(), late_loads[1].wait(), d2_arrived(7, 0), sum_sent(18), r_due(1)),
        lambda: (on_c(0), chunk_wait(FINAL + 2), d2_sent(0)),
        lambda: (d2_start(7, 2, 0), d2_arrived(7, 1), sum_sent(19), late_loads[2].wait()),
        lambda: (on_c(1), d2_sent(1), r_due(2)),
        lambda: (d2_start(8, 0, 1), d2_arrived(7, 2), sum_sent(20), late_loads[3].wait()),
        lambda: d2_sent(0),
        lambda: (d2_start(8, 1, 0), d2_sent(1), on_c(2)),
        lambda: (d2_start(8, 2, 1), d2_arrived(8, 0), rs_arrived(7, 0), late_loads[4].wait(), late_loads[5].wait()),
        lambda: (d2_arrived(8, 1), rs_arrived(7, 1)),
    )

    def late(t, _):
        for lo, hi in ((0, 4), (4, 8), (8, 11)):
            @_when((t >= lo) & (t < hi))
            def _():
                for i in range(lo, hi):
                    _when(t == i)(tops[i])

        w_c = (t == 2) | (t == 4) | (t == 6)
        w_0 = t > 8
        o = jnp.where(t < 2, t, jnp.where(t == 3, 2, jnp.where(t == 5, 3, t - 3)))
        g = jnp.where(w_c, t // 2 - 1, jnp.where(w_0, t - 9, lax.rem(o, 3)))
        s = lax.rem(FINAL + g, RING)

        @pl.when(jnp.logical_not(w_c | w_0))
        def _():
            def store(i, v):
                d2s[lax.rem(o, 2), :, pl.ds(i * T, T)] = v.astype(BF16)

            group(s, g, jnp.where(o < 3, 1, 0), 0, store)

        for cond, n, terms in ((w_c, 7, terms_c), (w_0, 8, terms_0)):
            @pl.when(cond)
            def _():
                group(s, g, 8 - n, 1, lambda i, v: add(n, g, terms, i, v))

        return 0

    lax.fori_loop(0, 11, late, 0)

    last = 2
    d2_arrived(8, last)

    def keep(i, v):
        cols = pl.ds(last * V + i * T, T)
        accbuf[:, cols] = v

    group((FINAL + last) % RING, last, 0, 1, keep)
    rs_arrived(7, last)
    for i in range(6):
        add(8, last, terms_0, i)

    d2_sent(0)
    d2_sent(1)
    await_bytes(xall.at[:, 0], ag_send.at[0])
    await_bytes(xall.at[pl.ds(0, 4)], ag_send.at[1])
    for s in range(LS):
        sum_sent(s)


def _call(x, wg, wu, wd):
    dma = pltpu.SemaphoreType.DMA
    rows = (ROWS, D)
    return pl.pallas_call(
        _kernel,
        out_shape=(
            pltpu.VMEM(rows, BF16),
            *(pltpu.HBM(shape, BF16) for shape in ((7, 2, *rows), (6, *rows))),
        ),
        in_specs=[pl.BlockSpec(memory_space=pltpu.HBM)] * 4,
        out_specs=[pl.BlockSpec(memory_space=m) for m in (pltpu.VMEM, pltpu.HBM, pltpu.HBM)],
        scratch_shapes=[
            pltpu.VMEM((2, 2 * ROWS, D), BF16),
            pltpu.VMEM((4, *rows), BF16),
            pltpu.VMEM((RING, F, V), BF16),
            pltpu.VMEM(rows, F32),
            pltpu.VMEM((2, ROWS, V), BF16),
            pltpu.VMEM((LS, ROWS, V), BF16),
            pltpu.VMEM(rows, BF16),
            pltpu.VMEM(rows, BF16),
            pltpu.VMEM((2, ROWS, T), F32),
            *(dma(s) for s in ((RING,), (3,), (2,), (6,), (2,), (7, 2), (8, 2), (2,), (2, 3), (LS,), (7, 3))),
        ],
        compiler_params=pltpu.CompilerParams(
            collective_id=0, has_side_effects=True, vmem_limit_bytes=64_500_000
        ),
        name="mlp",
    )(x, wg, wu, wd)[0]


def solution(mesh):
    return jax.shard_map(
        _call,
        mesh=mesh,
        in_specs=(P(("dp", "tp"), None), P(None, "tp"), P(None, "tp"), P("tp", None)),
        out_specs=P(("dp", "tp"), None),
        check_vma=False,
    )
```

```python
import functools

import jax
import jax.numpy as jnp
from jax import lax
from jax.experimental import pallas as pl
from jax.experimental.pallas import tpu as pltpu
from jax.sharding import PartitionSpec as P

MESH = pl.DeviceIdType.MESH
F32, BF16 = jnp.float32, jnp.bfloat16

ROWS = 256
D = 4608
F = 2304
T = 256
KA, KB = D // T, F // T
W = 3 * T
V = 6 * T
CH = D // 2
PARTS = ((0, 96), (96, 80), (176, 80))
RING = 4
EARLY = 12
FINAL = 66
LS = 2
SLICE = 16
A, B, C = range(3)


def _gelu_mul(g, u):
    t = jnp.tanh(0.7978845608028654 * (g + 0.044715 * (g * g * g)))
    return (g * (0.5 * (1.0 + t)) * u).astype(BF16)


def _when(cond):
    def run(f):
        def trip(_, carry):
            f()
            return carry

        lax.fori_loop(0, jnp.where(cond, 1, 0), trip, 0)

    return run


def _kernel(
    x, wg, wu, wd, y, xall, rbuf,
    xbuf, hub, ring, accbuf, d2s, pair,
    w_sem, f_sem, x_sem, r_sem, ag_send, ag_recv, ad_recv, ds_sem, dr_sem, ls_sem, rs_recv,
):
    me = lax.axis_index("tp")
    core = lax.rem(me, 2)
    partner = me + 1 - 2 * core
    axes = [me + m * (1 - 2 * lax.rem(me // m, 2)) for m in (8, 4, 2)]
    nbr = [
        [jnp.where(core == 0, axes[(p + r) % 3], axes[(p + r + 1) % 3]) for r in range(3)]
        for p in range(3)
    ]

    def local(src, dst, sem):
        return pltpu.make_async_copy(src, dst, sem)

    def await_bytes(ref, sem):
        pltpu.make_async_copy(ref, ref, sem).wait()

    def remote(src, dst, send, recv, to):
        return pltpu.make_async_remote_copy(
            src_ref=src, dst_ref=dst, send_sem=send, recv_sem=recv,
            device_id={"tp": to}, device_id_type=MESH,
        )

    def load_one(w, i, p):
        s = lax.rem(p, RING)
        cols = pl.ds(pl.multiple_of(i * W, T), W)
        for d in range(2):
            local(
                w.at[pl.ds(d * F, F), cols], ring.at[s, :, pl.ds(d * W, W)], w_sem.at[s]
            ).start()

    def load_pair(i, p):
        load_one(wg, i, p)
        load_one(wu, i, p + 1)

    def load_down(j, p):
        s = lax.rem(p, RING)
        local(wd.at[:, pl.ds(j * V, V)], ring.at[s], w_sem.at[s]).start()

    def chunk_wait(p):
        s = lax.rem(p, RING)
        await_bytes(ring.at[s], w_sem.at[s])

    def product(lhs, rhs, depth):
        total = None
        for k in range(depth):
            t = jnp.dot(lhs(k), rhs(k), preferred_element_type=F32)
            total = t if total is None else total + t
        return total

    def tile_a(p, xs, row, i, hb, half, j, extra=None):
        sl = [lax.rem(p + q, RING) for q in range(2)]

        def lhs(k):
            return xbuf[xs, pl.ds(row, ROWS), pl.ds(k * T, T)]

        def rhs(q):
            def tile(k):
                at = pl.multiple_of((k // KB) * W + i * T, T) if not isinstance(i, int) else (k // KB) * W + i * T
                return ring[sl[q], pl.ds((k % KB) * T, T), pl.ds(at, T)]

            return tile

        g, u = product(lhs, rhs(0), KA), product(lhs, rhs(1), KA)
        cols = pl.ds(pl.multiple_of(half * F + j * T, T), T)
        if extra is None:
            hub[hb, :, cols] = _gelu_mul(g, u)
            return
        pair[0], pair[1] = g, u
        for r in range(0, ROWS, SLICE):
            rows = pl.ds(r, SLICE)
            extra(r)
            hub[hb, rows, cols] = _gelu_mul(pair[0, rows], pair[1, rows])

    def step_a(p, xs, hb, flip, e, extra=None):
        for i in range(3):
            for h in range(2):
                tile_a(
                    p, xs, h * ROWS, i, hb, jnp.where(flip, 1 - h, h), 3 * e + i,
                    extra and functools.partial(extra, 2 * i + h),
                )

    def step_b(p, j, slot):
        s = lax.rem(p, RING)
        for i in range(6):
            d2s[slot, :, pl.ds(i * T, T)] = rows_b(1, 0, i, s).astype(BF16)
            accbuf[:, pl.ds(pl.multiple_of(j * V + i * T, T), T)] = rows_b(1, 1, i, s)

    def rows_b(hb, h, i, s):
        def lhs(k):
            return hub[hb, :, pl.ds(h * F + k * T, T)]

        def rhs(k):
            return ring[s, pl.ds(k * T, T), pl.ds(i * T, T)]

        return product(lhs, rhs, KB)

    def ag_start(src, dst, role, c):
        cols = pl.ds(c * CH, CH)
        for p, (o, n) in enumerate(PARTS):
            rows = pl.ds(o, n)
            remote(
                x.at[rows, cols] if src == 0 else xall.at[src - 1, 0, rows, cols],
                xall.at[dst - 1, 0, rows, cols],
                ag_send.at[0],
                ag_recv.at[dst - 1, c],
                nbr[p][role],
            ).start()

    def ag_arrived(n, c):
        await_bytes(xall.at[n - 1, 0, :, pl.ds(c * CH, CH)], ag_recv.at[n - 1, c])

    def pass_on(n, c):
        cols = pl.ds(c * CH, CH)
        if n < 2:
            dst = xbuf.at[n, pl.ds((1 - n) * ROWS, ROWS), cols]
        else:
            dst = xall.at[n - 1, 1, :, cols]
        src = x.at[:, cols] if n == 0 else xall.at[n - 1, 0, :, cols]
        remote(src, dst, ag_send.at[1], ad_recv.at[n, c], partner).start()

    def passed(n, c):
        await_bytes(x.at[:, pl.ds(0, CH)], ad_recv.at[n, c])

    def relay(n):
        for c in range(2):
            ag_arrived(n, c)
            pass_on(n, c)

    def x_load(n):
        xs = lax.rem(n, 2)
        return [
            local(xall.at[n - 1, 1 - h], xbuf.at[xs, pl.ds(h * ROWS, ROWS)], x_sem.at[h])
            for h in range(2)
        ]

    def own_load(c):
        cols = pl.ds(c * CH, CH)
        return local(xall.at[0, 0, :, cols], xbuf.at[1, pl.ds(ROWS, ROWS), cols], x_sem.at[c])

    def cols_of(j):
        return pl.ds(pl.multiple_of(j * V, T), V)

    def d2_start(n, j, slot):
        remote(
            d2s.at[slot],
            hub.at[2 + lax.rem(n, 2), :, cols_of(j)],
            ds_sem.at[slot],
            dr_sem.at[lax.rem(n, 2), j],
            partner,
        ).start()

    def d2_sent(slot):
        await_bytes(d2s.at[slot], ds_sem.at[slot])

    def d2_arrived(n, j):
        await_bytes(d2s.at[0], dr_sem.at[lax.rem(n, 2), j])

    def out_at(h, rows, col, width):
        return 4, rows, pl.ds(pl.multiple_of(h * CH + col, T), width)

    def sum_start(n, j, to, src, sem, width, dst):
        cols = pl.ds(pl.multiple_of(j * width, T), width)
        for p, (o, rows) in enumerate(PARTS):
            remote(
                src(pl.ds(o, rows)),
                dst.at[pl.ds(o, rows), cols],
                sem,
                rs_recv.at[n - 1, j],
                to(p),
            ).start()

    def sum_on(n, h):
        sum_start(
            n, h, lambda p: jnp.where(n < 5, nbr[p][A], nbr[p][B]),
            lambda rows: hub.at[out_at(h, rows, 0, CH)], ls_sem.at[h], CH, rbuf.at[n - 1],
        )

    def sum_sent(slot, width):
        await_bytes(xbuf.at[0, pl.ds(0, ROWS), pl.ds(0, width)], ls_sem.at[slot])

    def rs_arrived(n, j):
        width = V if isinstance(n, int) and n == 7 else CH
        await_bytes(xbuf.at[0, pl.ds(0, ROWS), pl.ds(0, width)], rs_recv.at[n - 1, j])

    def add_rows(n, t, terms, r, dst, value=None):
        size = SLICE if value is None else ROWS
        cols = pl.ds(pl.multiple_of(t * T, T), T)
        rows = pl.ds(r, size)
        v = accbuf[rows, cols] if value is None else value
        if n is not None:
            v = v + hub[2 + lax.rem(n, 2), rows, cols].astype(F32)
        for ref, r0 in terms:
            v = v + ref[pl.ds(r0 + r, size), cols].astype(F32)
        dst(rows, v)

    terms_c = ((xbuf.at[0], 0), (xbuf.at[1], ROWS))
    terms_0 = ((hub.at[5], 0), (xbuf.at[1], 0), (y, 0))

    def r_load(i, src, dst, col=0, width=D):
        cols = pl.ds(col, width)
        h, r = dst
        return local(rbuf.at[src - 1, :, cols], xbuf.at[h, pl.ds(r, ROWS), cols], r_sem.at[i])

    late_loads = (
        r_load(0, 3, (0, 0)), *(r_load(1 + k, 6, (1, ROWS), k * CH, CH) for k in range(2)),
        local(rbuf.at[0], hub.at[5], r_sem.at[3]), r_load(4, 5, (1, 0)),
    )

    def first_tile(i):
        for q, w in enumerate((wg, wu)):
            for d in range(2):
                local(
                    w.at[pl.ds(d * F, F), pl.ds(i * T, T)],
                    ring.at[q, :, pl.ds(d * W + i * T, T)],
                    f_sem.at[i],
                ).start()

    own = local(x, xbuf.at[0, pl.ds(0, ROWS)], x_sem.at[0])
    own.start()
    first_tile(0)
    barrier = pltpu.get_barrier_semaphore()
    for d in (*axes, partner):
        pl.semaphore_signal(barrier, inc=1, device_id={"tp": d}, device_id_type=MESH)
    hub[5] = jnp.zeros_like(hub[5])
    first_tile(1)
    pl.semaphore_wait(barrier, 4)
    for c in range(2):
        pass_on(0, c)
    for c in range(2):
        ag_start(0, 1, A, c)
    own.wait()

    def piece(i, _):
        await_bytes(ring.at[0, :, pl.ds(0, 4 * T)], f_sem.at[i])
        _when(i == 0)(lambda: first_tile(2))
        _when(i == 1)(lambda: load_pair(1, 2))
        tile_a(0, 0, 0, i, 0, 1, i)
        return 0

    lax.fori_loop(0, 3, piece, 0)

    def third(m, _):
        @_when(m == 0)
        def _():
            passed(0, 0)
            passed(0, 1)

        @_when(m > 0)
        def _():
            @_when(m == 1)
            def _():
                for q in range(2):
                    chunk_wait(4 + q)
                load_pair(0, 6)

            for c in range(2):
                @_when(m == 1 + c)
                def _():
                    ag_arrived(1, c)
                    pass_on(1, c)
                    own_load(c).start()
                    ag_start(1, 2, B, c)
                    if c:
                        ag_start(1, 3, C, 0)
                        ag_start(1, 3, C, 1)

        h = jnp.where(m == 1, 0, 1)
        e = jnp.where(m == 0, 0, 2)
        for i in range(3):
            tile_a(2 * e, 0, pl.multiple_of(h * ROWS, ROWS), i, 0, 1 - h, 3 * e + i)
        return 0

    def third_hop(c):
        ag_arrived(2, c)
        pass_on(2, c)
        ag_start(2, 4, C, c)

    def early(e, _):
        p = 2 * e
        chunk_wait(p)
        chunk_wait(p + 1)

        @_when(e < 5)
        def _():
            load_pair(lax.rem(e + 1, 3), p + 2)

        @_when(e >= 3)
        def _():
            @_when(e == 3)
            def _():
                for c in range(2):
                    passed(1, c)
                    own_load(c).wait()

            _when(e == 4)(lambda: third_hop(0))

            @_when(e == 5)
            def _():
                for i in range(2):
                    load_down(i, EARLY + i)

        n = e // 3
        step_a(p, n, n, n == 0, lax.rem(e, 3))
        return 0

    def opening(g, _):
        lax.fori_loop(g, 2 * g + 1, third, 0)
        lax.fori_loop(2 * g + 1, 4 * g + 2, early, 0)
        return 0

    lax.fori_loop(0, 2, opening, 0)

    def block(n, _):
        base = EARLY + 9 * (n - 1)

        def down(j, _):
            p = base + j
            slot = lax.rem(n + j, 2)
            chunk_wait(p)

            @_when(j > 0)
            def _():
                d2_start(n, j - 1, 1 - slot)
                _when(j == 2)(lambda: load_one(wg, 1, p + 3))

                @_when(j == 1)
                def _():
                    load_one(wu, 0, p + 3)
                    passed(n + 1, 0)
                    passed(n + 1, 1)
                    for copy in x_load(n + 1):
                        copy.start()

            @pl.when((n > 1) | (j > 1))
            def _():
                d2_sent(slot)

            @_when(j == 0)
            def _():
                load_down(2, p + 2)
                load_one(wg, 0, p + 3)

                _when(n == 1)(lambda: third_hop(1))

                for m, role in ((1, B), (3, C)):
                    @_when(n == m)
                    def _():
                        for c in range(2):
                            ag_start(0, m + 4, role, c)

                for m, blk in ((2, 4), (4, 6), (5, 7)):
                    _when(n == m)(functools.partial(relay, blk))

                for m, src in ((5, 2), (6, 4)):
                    @_when(n == m)
                    def _():
                        for i in range(2):
                            rs_arrived(src, i)
                        local(rbuf.at[src - 1], hub.at[5], r_sem.at[0]).start()

            step_b(p, j, slot)
            return 0

        lax.fori_loop(0, 3, down, 0)

        xs = lax.rem(n + 1, 2)

        def gate_up(j, _):
            p = base + 3 + 2 * j
            chunk_wait(p)
            chunk_wait(p + 1)

            @_when(j == 0)
            def _():
                d2_start(n, 2, lax.rem(n, 2))
                load_one(wu, 1, p + 3)
                for copy in x_load(n + 1):
                    copy.wait()

                @pl.when(n > 4)
                def _():
                    local(rbuf.at[0], hub.at[5], r_sem.at[0]).wait()

                _when(n == 1)(lambda: relay(3))

                @_when(n == 2)
                def _():
                    relay(5)
                    for c in range(2):
                        ag_start(5, 6, C, c)

                d2_arrived(n, 0)

            @_when(j == 1)
            def _():
                sum_on(n, 0)
                load_pair(2, p + 2)

            pl.when(n > 1)(lambda: sum_sent(j, CH))
            d2_arrived(n, j + 1)

            def extra(i, r):
                q = (i * ROWS + r) // SLICE
                for k in range(9 * q // 5, 9 * (q + 1) // 5):
                    t, row = divmod(k * SLICE, ROWS)
                    if t < 9:

                        def dst(rows, v, t=t):
                            hub[out_at(j, rows, t * T, T)] = v.astype(BF16)

                        add_rows(n, 9 * j + t, ((hub.at[5], 0),), row, dst)

            step_a(p, xs, 1, False, j, extra)
            return 0

        lax.fori_loop(0, 2, gate_up, 0)
        p = base + 7
        chunk_wait(p)
        chunk_wait(p + 1)
        sum_on(n, 1)
        for i in range(2):
            load_down(i, p + 2 + i)
        step_a(p, xs, 1, False, 2)
        return 0

    lax.fori_loop(1, 7, block, 0)

    def group(s, g, hb, h, store):
        for i in range(6):
            store(i, rows_b(hb, h, i, s))

    def c_sums(rows, cols):
        return xbuf.at[0, pl.ds(ROWS + rows.start, rows.size), cols]

    def on_c(j):
        sum_start(
            7, j, lambda p: nbr[p][C], lambda rows: c_sums(rows, cols_of(j)), ls_sem.at[LS + j], V, y
        )

    def r_due(k):
        rs_arrived(6, k)
        late_loads[1 + k].start()

    tops = (
        lambda: (load_down(2, FINAL + 2), chunk_wait(FINAL), d2_sent(0), d2_sent(1),
                 [rs_arrived(n, k) for n in (1, 3, 5) for k in range(2)], r_due(0),
                 [late_loads[i].start() for i in (0, 3, 4)]),
        lambda: (d2_start(7, 0, 0), chunk_wait(FINAL + 1)),
        lambda: (d2_start(7, 1, 1), late_loads[0].wait(), late_loads[1].wait(), d2_arrived(7, 0)),
        lambda: (on_c(0), chunk_wait(FINAL + 2), d2_sent(0), r_due(1)),
        lambda: (d2_start(7, 2, 0), d2_arrived(7, 1), late_loads[2].wait()),
        lambda: (on_c(1), d2_sent(1)),
        lambda: (d2_start(8, 0, 1), d2_arrived(7, 2)),
        lambda: d2_sent(0),
        lambda: (d2_start(8, 1, 0), d2_sent(1), on_c(2)),
        lambda: (d2_start(8, 2, 1), d2_arrived(8, 0), rs_arrived(7, 0), late_loads[3].wait(), late_loads[4].wait()),
        lambda: (d2_arrived(8, 1), rs_arrived(7, 1)),
    )

    def late(t, _):
        for lo, hi in ((0, 4), (4, 8), (8, 11)):
            @_when((t >= lo) & (t < hi))
            def _():
                for i in range(lo, hi):
                    _when(t == i)(tops[i])

        w_c = (t == 2) | (t == 4) | (t == 6)
        w_0 = t > 8
        o = jnp.where(t < 2, t, jnp.where(t == 3, 2, jnp.where(t == 5, 3, t - 3)))
        g = jnp.where(w_c, t // 2 - 1, jnp.where(w_0, t - 9, lax.rem(o, 3)))
        s = lax.rem(FINAL + g, RING)

        @pl.when(jnp.logical_not(w_c | w_0))
        def _():
            def store(i, v):
                d2s[lax.rem(o, 2), :, pl.ds(i * T, T)] = v.astype(BF16)

            group(s, g, jnp.where(o < 3, 1, 0), 0, store)

        for cond, n, terms in ((w_c, 7, terms_c), (w_0, 8, terms_0)):
            @pl.when(cond)
            def _():
                def store(i, v):
                    cols = pl.ds(pl.multiple_of(g * V + i * T, T), T)

                    def dst(rows, v):
                        if n == 7:
                            xbuf[0, pl.ds(ROWS, ROWS), cols] = v.astype(BF16)
                        else:
                            y[rows, cols] = v.astype(BF16)

                    add_rows(n, 6 * g + i, terms, 0, dst, v)

                group(s, g, 8 - n, 1, store)

        return 0

    lax.fori_loop(0, 11, late, 0)

    last = 2
    d2_arrived(8, last)

    def keep(i, v):
        cols = pl.ds(last * V + i * T, T)

        def dst(rows, v):
            accbuf[rows, cols] = v

        add_rows(8, 6 * last + i, terms_0[:2], 0, dst, v)

    group((FINAL + last) % RING, last, 0, 1, keep)
    rs_arrived(7, last)
    for i in range(6):
        cols = pl.ds(last * V + i * T, T)

        def dst(rows, v, cols=cols):
            y[rows, cols] = v.astype(BF16)

        for r in range(0, ROWS, SLICE):
            add_rows(None, 6 * last + i, terms_0[2:], r, dst)

    d2_sent(0)
    d2_sent(1)
    await_bytes(xall.at[:, 0], ag_send.at[0])
    await_bytes(xall.at[pl.ds(0, 4)], ag_send.at[1])
    for s in range(LS):
        sum_sent(s, CH)
    for s in range(3):
        sum_sent(LS + s, V)


def _call(x, wg, wu, wd):
    dma = pltpu.SemaphoreType.DMA
    rows = (ROWS, D)
    return pl.pallas_call(
        _kernel,
        out_shape=(
            pltpu.VMEM(rows, BF16),
            *(pltpu.HBM(shape, BF16) for shape in ((7, 2, *rows), (6, *rows))),
        ),
        in_specs=[pl.BlockSpec(memory_space=pltpu.HBM)] * 4,
        out_specs=[pl.BlockSpec(memory_space=m) for m in (pltpu.VMEM, pltpu.HBM, pltpu.HBM)],
        scratch_shapes=[
            pltpu.VMEM((2, 2 * ROWS, D), BF16),
            pltpu.VMEM((6, *rows), BF16),
            pltpu.VMEM((RING, F, V), BF16),
            pltpu.VMEM(rows, F32),
            pltpu.VMEM((2, ROWS, V), BF16),
            pltpu.VMEM((2, ROWS, T), F32),
            *(dma(s) for s in ((RING,), (3,), (2,), (5,), (2,), (7, 2), (8, 2), (2,), (2, 3), (LS + 3,), (7, 3))),
        ],
        compiler_params=pltpu.CompilerParams(
            collective_id=0, has_side_effects=True, vmem_limit_bytes=64_500_000
        ),
        name="mlp",
    )(x, wg, wu, wd)[0]


def solution(mesh):
    return jax.shard_map(
        _call,
        mesh=mesh,
        in_specs=(P(("dp", "tp"), None), P(None, "tp"), P(None, "tp"), P("tp", None)),
        out_specs=P(("dp", "tp"), None),
        check_vma=False,
    )
```

```python
import functools

import jax
import jax.numpy as jnp
from jax import lax
from jax.experimental import pallas as pl
from jax.experimental.pallas import tpu as pltpu
from jax.sharding import PartitionSpec as P

MESH = pl.DeviceIdType.MESH
F32, BF16 = jnp.float32, jnp.bfloat16

ROWS = 256
D = 4608
F = 2304
T = 256
KA, KB = D // T, F // T
W = 3 * T
V = 6 * T
CH = D // 2
PARTS = ((0, 96), (96, 80), (176, 80))
RING = 4
EARLY = 12
FINAL = 66
LS = 2
SLICE = 16
A, B, C = range(3)


def _gelu_mul(g, u):
    t = jnp.tanh(0.7978845608028654 * (g + 0.044715 * (g * g * g)))
    return (g * (0.5 * (1.0 + t)) * u).astype(BF16)


def _when(cond):
    def run(f):
        def trip(_, carry):
            f()
            return carry

        lax.fori_loop(0, jnp.where(cond, 1, 0), trip, 0)

    return run


def _kernel(
    x, wg, wu, wd, y, xall, rbuf,
    xbuf, hub, ring, accbuf, d2s, pair,
    w_sem, f_sem, x_sem, r_sem, ag_send, ag_recv, ad_recv, ds_sem, dr_sem, ls_sem, rs_recv,
):
    me = lax.axis_index("tp")
    core = lax.rem(me, 2)
    partner = me + 1 - 2 * core
    axes = [me + m * (1 - 2 * lax.rem(me // m, 2)) for m in (8, 4, 2)]
    nbr = [
        [jnp.where(core == 0, axes[(p + r) % 3], axes[(p + r + 1) % 3]) for r in range(3)]
        for p in range(3)
    ]

    def local(src, dst, sem):
        return pltpu.make_async_copy(src, dst, sem)

    def await_bytes(ref, sem):
        pltpu.make_async_copy(ref, ref, sem).wait()

    def remote(src, dst, send, recv, to):
        return pltpu.make_async_remote_copy(
            src_ref=src, dst_ref=dst, send_sem=send, recv_sem=recv,
            device_id={"tp": to}, device_id_type=MESH,
        )

    def load_one(w, i, p):
        s = lax.rem(p, RING)
        cols = pl.ds(pl.multiple_of(i * W, T), W)
        for d in range(2):
            local(
                w.at[pl.ds(d * F, F), cols], ring.at[s, :, pl.ds(d * W, W)], w_sem.at[s]
            ).start()

    def load_pair(i, p):
        load_one(wg, i, p)
        load_one(wu, i, p + 1)

    def load_down(j, p):
        s = lax.rem(p, RING)
        local(wd.at[:, pl.ds(j * V, V)], ring.at[s], w_sem.at[s]).start()

    def chunk_wait(p):
        s = lax.rem(p, RING)
        await_bytes(ring.at[s], w_sem.at[s])

    def product(lhs, rhs, depth):
        total = None
        for k in range(depth):
            t = jnp.dot(lhs(k), rhs(k), preferred_element_type=F32)
            total = t if total is None else total + t
        return total

    def tile_a(p, xs, row, i, hb, half, j, extra=None):
        sl = [lax.rem(p + q, RING) for q in range(2)]

        def lhs(k):
            return xbuf[xs, pl.ds(row, ROWS), pl.ds(k * T, T)]

        def rhs(q):
            def tile(k):
                at = pl.multiple_of((k // KB) * W + i * T, T) if not isinstance(i, int) else (k // KB) * W + i * T
                return ring[sl[q], pl.ds((k % KB) * T, T), pl.ds(at, T)]

            return tile

        g, u = product(lhs, rhs(0), KA), product(lhs, rhs(1), KA)
        cols = pl.ds(pl.multiple_of(half * F + j * T, T), T)
        if extra is None:
            hub[hb, :, cols] = _gelu_mul(g, u)
            return
        pair[0], pair[1] = g, u
        for r in range(0, ROWS, SLICE):
            rows = pl.ds(r, SLICE)
            extra(r)
            hub[hb, rows, cols] = _gelu_mul(pair[0, rows], pair[1, rows])

    def step_a(p, xs, hb, flip, e, extra=None):
        for i in range(3):
            for h in range(2):
                tile_a(
                    p, xs, h * ROWS, i, hb, jnp.where(flip, 1 - h, h), 3 * e + i,
                    extra and functools.partial(extra, 2 * i + h),
                )

    def step_b(p, j, slot):
        s = lax.rem(p, RING)
        for i in range(6):
            d2s[slot, :, pl.ds(i * T, T)] = rows_b(1, 0, i, s).astype(BF16)
            accbuf[:, pl.ds(pl.multiple_of(j * V + i * T, T), T)] = rows_b(1, 1, i, s)

    def rows_b(hb, h, i, s):
        def lhs(k):
            return hub[hb, :, pl.ds(h * F + k * T, T)]

        def rhs(k):
            return ring[s, pl.ds(k * T, T), pl.ds(i * T, T)]

        return product(lhs, rhs, KB)

    def ag_start(src, dst, role, c):
        cols = pl.ds(c * CH, CH)
        for p, (o, n) in enumerate(PARTS):
            rows = pl.ds(o, n)
            remote(
                x.at[rows, cols] if src == 0 else xall.at[src - 1, 0, rows, cols],
                xall.at[dst - 1, 0, rows, cols],
                ag_send.at[0],
                ag_recv.at[dst - 1, c],
                nbr[p][role],
            ).start()

    def ag_arrived(n, c):
        await_bytes(xall.at[n - 1, 0, :, pl.ds(c * CH, CH)], ag_recv.at[n - 1, c])

    def pass_on(n, c):
        cols = pl.ds(c * CH, CH)
        if n < 2:
            dst = xbuf.at[n, pl.ds((1 - n) * ROWS, ROWS), cols]
        else:
            dst = xall.at[n - 1, 1, :, cols]
        src = x.at[:, cols] if n == 0 else xall.at[n - 1, 0, :, cols]
        remote(src, dst, ag_send.at[1], ad_recv.at[n, c], partner).start()

    def passed(n, c):
        await_bytes(x.at[:, pl.ds(0, CH)], ad_recv.at[n, c])

    def relay(n):
        for c in range(2):
            ag_arrived(n, c)
            pass_on(n, c)

    def x_load(n):
        xs = lax.rem(n, 2)
        return [
            local(xall.at[n - 1, 1 - h], xbuf.at[xs, pl.ds(h * ROWS, ROWS)], x_sem.at[h])
            for h in range(2)
        ]

    def own_load(c):
        cols = pl.ds(c * CH, CH)
        return local(xall.at[0, 0, :, cols], xbuf.at[1, pl.ds(ROWS, ROWS), cols], x_sem.at[c])

    def cols_of(j):
        return pl.ds(pl.multiple_of(j * V, T), V)

    def d2_start(n, j, slot):
        remote(
            d2s.at[slot],
            hub.at[2 + lax.rem(n, 2), :, cols_of(j)],
            ds_sem.at[slot],
            dr_sem.at[lax.rem(n, 2), j],
            partner,
        ).start()

    def d2_sent(slot):
        await_bytes(d2s.at[slot], ds_sem.at[slot])

    def d2_arrived(n, j):
        await_bytes(d2s.at[0], dr_sem.at[lax.rem(n, 2), j])

    def out_at(h, rows, col, width):
        return 4, rows, pl.ds(pl.multiple_of(h * CH + col, T), width)

    def sum_start(n, j, to, src, sem, width, dst):
        cols = pl.ds(pl.multiple_of(j * width, T), width)
        for p, (o, rows) in enumerate(PARTS):
            remote(
                src(pl.ds(o, rows)),
                dst.at[pl.ds(o, rows), cols],
                sem,
                rs_recv.at[n - 1, j],
                to(p),
            ).start()

    def sum_on(n, h):
        sum_start(
            n, h, lambda p: jnp.where(n < 5, nbr[p][A], nbr[p][B]),
            lambda rows: hub.at[out_at(h, rows, 0, CH)], ls_sem.at[h], CH, rbuf.at[n - 1],
        )

    def sum_sent(slot, width):
        await_bytes(xbuf.at[0, pl.ds(0, ROWS), pl.ds(0, width)], ls_sem.at[slot])

    def rs_arrived(n, j):
        width = V if isinstance(n, int) and n == 7 else CH
        await_bytes(xbuf.at[0, pl.ds(0, ROWS), pl.ds(0, width)], rs_recv.at[n - 1, j])

    def add_rows(n, t, terms, r, dst, value=None):
        size = SLICE if value is None else ROWS
        cols = pl.ds(pl.multiple_of(t * T, T), T)
        rows = pl.ds(r, size)
        v = accbuf[rows, cols] if value is None else value
        if n is not None:
            v = v + hub[2 + lax.rem(n, 2), rows, cols].astype(F32)
        for ref, r0 in terms:
            v = v + ref[pl.ds(r0 + r, size), cols].astype(F32)
        dst(rows, v)

    terms_c = ((xbuf.at[0], 0), (xbuf.at[1], ROWS))
    terms_0 = ((hub.at[5], 0), (xbuf.at[1], 0), (y, 0))

    def r_load(i, src, dst, col=0, width=D):
        cols = pl.ds(col, width)
        h, r = dst
        return local(rbuf.at[src - 1, :, cols], xbuf.at[h, pl.ds(r, ROWS), cols], r_sem.at[i])

    late_loads = (
        r_load(0, 3, (0, 0)), *(r_load(1 + k, 6, (1, ROWS), k * CH, CH) for k in range(2)),
        local(rbuf.at[0], hub.at[5], r_sem.at[3]), r_load(4, 5, (1, 0)),
    )

    def first_tile(i):
        for q, w in enumerate((wg, wu)):
            for d in range(2):
                local(
                    w.at[pl.ds(d * F, F), pl.ds(i * T, T)],
                    ring.at[q, :, pl.ds(d * W + i * T, T)],
                    f_sem.at[i],
                ).start()

    own = local(x, xbuf.at[0, pl.ds(0, ROWS)], x_sem.at[0])
    own.start()
    first_tile(0)
    barrier = pltpu.get_barrier_semaphore()
    for d in (*axes, partner):
        pl.semaphore_signal(barrier, inc=1, device_id={"tp": d}, device_id_type=MESH)
    hub[5] = jnp.zeros_like(hub[5])
    first_tile(1)
    pl.semaphore_wait(barrier, 4)
    for c in range(2):
        pass_on(0, c)
    for c in range(2):
        ag_start(0, 1, A, c)
    own.wait()

    def piece(i, _):
        await_bytes(ring.at[0, :, pl.ds(0, 4 * T)], f_sem.at[i])
        _when(i == 0)(lambda: first_tile(2))
        _when(i == 1)(lambda: load_pair(1, 2))
        tile_a(0, 0, 0, i, 0, 1, i)
        return 0

    lax.fori_loop(0, 3, piece, 0)

    def third(m, _):
        @_when(m == 0)
        def _():
            passed(0, 0)
            passed(0, 1)

        @_when(m > 0)
        def _():
            @_when(m == 1)
            def _():
                for q in range(2):
                    chunk_wait(4 + q)
                load_pair(0, 6)

            for c in range(2):
                @_when(m == 1 + c)
                def _():
                    ag_arrived(1, c)
                    pass_on(1, c)
                    own_load(c).start()
                    ag_start(1, 2, B, c)
                    if c:
                        ag_start(1, 3, C, 0)
                        ag_start(1, 3, C, 1)

        h = jnp.where(m == 1, 0, 1)
        e = jnp.where(m == 0, 0, 2)
        for i in range(3):
            tile_a(2 * e, 0, pl.multiple_of(h * ROWS, ROWS), i, 0, 1 - h, 3 * e + i)
        return 0

    def third_hop(c):
        ag_arrived(2, c)
        pass_on(2, c)
        ag_start(2, 4, C, c)

    def early(e, _):
        p = 2 * e
        chunk_wait(p)
        chunk_wait(p + 1)

        @_when(e < 5)
        def _():
            load_pair(lax.rem(e + 1, 3), p + 2)

        @_when(e >= 3)
        def _():
            @_when(e == 3)
            def _():
                for c in range(2):
                    passed(1, c)
                    own_load(c).wait()

            _when(e == 4)(lambda: third_hop(0))

            @_when(e == 5)
            def _():
                for i in range(2):
                    load_down(i, EARLY + i)

        n = e // 3
        step_a(p, n, n, n == 0, lax.rem(e, 3))
        return 0

    def opening(g, _):
        lax.fori_loop(g, 2 * g + 1, third, 0)
        lax.fori_loop(2 * g + 1, 4 * g + 2, early, 0)
        return 0

    lax.fori_loop(0, 2, opening, 0)

    def block(n, _):
        base = EARLY + 9 * (n - 1)

        def down(j, _):
            p = base + j
            slot = lax.rem(n + j, 2)
            chunk_wait(p)

            @_when(j > 0)
            def _():
                d2_start(n, j - 1, 1 - slot)
                _when(j == 2)(lambda: load_one(wg, 1, p + 3))

                @_when(j == 1)
                def _():
                    load_one(wu, 0, p + 3)
                    passed(n + 1, 0)
                    passed(n + 1, 1)
                    for copy in x_load(n + 1):
                        copy.start()

            @pl.when((n > 1) | (j > 1))
            def _():
                d2_sent(slot)

            @_when(j == 0)
            def _():
                load_down(2, p + 2)
                load_one(wg, 0, p + 3)

                _when(n == 1)(lambda: third_hop(1))

                for m, blk, role in ((2, 5, B), (4, 7, C)):
                    @_when(n == m)
                    def _():
                        for c in range(2):
                            ag_start(0, blk, role, c)

                _when(n == 2)(lambda: relay(4))

                @_when(n == 3)
                def _():
                    relay(5)
                    for c in range(2):
                        ag_start(5, 6, C, c)

                for m, src in ((5, 2), (6, 4)):
                    @_when(n == m)
                    def _():
                        for i in range(2):
                            rs_arrived(src, i)
                        local(rbuf.at[src - 1], hub.at[5], r_sem.at[0]).start()

            step_b(p, j, slot)
            return 0

        lax.fori_loop(0, 3, down, 0)

        xs = lax.rem(n + 1, 2)

        def gate_up(j, _):
            p = base + 3 + 2 * j
            chunk_wait(p)
            chunk_wait(p + 1)

            @_when(j == 0)
            def _():
                d2_start(n, 2, lax.rem(n, 2))
                load_one(wu, 1, p + 3)
                for copy in x_load(n + 1):
                    copy.wait()

                @pl.when(n > 4)
                def _():
                    local(rbuf.at[0], hub.at[5], r_sem.at[0]).wait()

                _when(n == 1)(lambda: relay(3))

                d2_arrived(n, 0)

            @_when(j == 1)
            def _():
                sum_on(n, 0)
                load_pair(2, p + 2)

            pl.when(n > 1)(lambda: sum_sent(j, CH))
            d2_arrived(n, j + 1)

            def extra(i, r):
                q = (i * ROWS + r) // SLICE
                for k in range(9 * q // 5, 9 * (q + 1) // 5):
                    t, row = divmod(k * SLICE, ROWS)
                    if t < 9:

                        def dst(rows, v, t=t):
                            hub[out_at(j, rows, t * T, T)] = v.astype(BF16)

                        add_rows(n, 9 * j + t, ((hub.at[5], 0),), row, dst)

            step_a(p, xs, 1, False, j, extra)
            return 0

        lax.fori_loop(0, 2, gate_up, 0)
        p = base + 7
        chunk_wait(p)
        chunk_wait(p + 1)
        sum_on(n, 1)
        for i in range(2):
            load_down(i, p + 2 + i)

        for m, blk in ((4, 6), (5, 7)):
            _when(n == m)(functools.partial(relay, blk))

        step_a(p, xs, 1, False, 2)
        return 0

    lax.fori_loop(1, 7, block, 0)

    def group(s, g, hb, h, store):
        for i in range(6):
            store(i, rows_b(hb, h, i, s))

    def c_sums(rows, cols):
        return xbuf.at[0, pl.ds(ROWS + rows.start, rows.size), cols]

    def on_c(j):
        sum_start(
            7, j, lambda p: nbr[p][C], lambda rows: c_sums(rows, cols_of(j)), ls_sem.at[LS + j], V, y
        )

    def r_due(k):
        rs_arrived(6, k)
        late_loads[1 + k].start()

    tops = (
        lambda: (load_down(2, FINAL + 2), chunk_wait(FINAL), d2_sent(0), d2_sent(1),
                 [rs_arrived(n, k) for n in (1, 3, 5) for k in range(2)], r_due(0),
                 [late_loads[i].start() for i in (0, 3, 4)]),
        lambda: (d2_start(7, 0, 0), chunk_wait(FINAL + 1)),
        lambda: (d2_start(7, 1, 1), late_loads[0].wait(), late_loads[1].wait(), d2_arrived(7, 0)),
        lambda: (on_c(0), chunk_wait(FINAL + 2), d2_sent(0), r_due(1)),
        lambda: (d2_start(7, 2, 0), d2_arrived(7, 1), late_loads[2].wait()),
        lambda: (on_c(1), d2_sent(1)),
        lambda: (d2_start(8, 0, 1), d2_arrived(7, 2)),
        lambda: d2_sent(0),
        lambda: (d2_start(8, 1, 0), d2_sent(1), on_c(2)),
        lambda: (d2_start(8, 2, 1), d2_arrived(8, 0), rs_arrived(7, 0), late_loads[3].wait(), late_loads[4].wait()),
        lambda: (d2_arrived(8, 1), rs_arrived(7, 1)),
    )

    def late(t, _):
        for lo, hi in ((0, 4), (4, 8), (8, 11)):
            @_when((t >= lo) & (t < hi))
            def _():
                for i in range(lo, hi):
                    _when(t == i)(tops[i])

        w_c = (t == 2) | (t == 4) | (t == 6)
        w_0 = t > 8
        o = jnp.where(t < 2, t, jnp.where(t == 3, 2, jnp.where(t == 5, 3, t - 3)))
        g = jnp.where(w_c, t // 2 - 1, jnp.where(w_0, t - 9, lax.rem(o, 3)))
        s = lax.rem(FINAL + g, RING)

        @pl.when(jnp.logical_not(w_c | w_0))
        def _():
            def store(i, v):
                d2s[lax.rem(o, 2), :, pl.ds(i * T, T)] = v.astype(BF16)

            group(s, g, jnp.where(o < 3, 1, 0), 0, store)

        for cond, n, terms in ((w_c, 7, terms_c), (w_0, 8, terms_0)):
            @pl.when(cond)
            def _():
                def store(i, v):
                    cols = pl.ds(pl.multiple_of(g * V + i * T, T), T)

                    def dst(rows, v):
                        if n == 7:
                            xbuf[0, pl.ds(ROWS, ROWS), cols] = v.astype(BF16)
                        else:
                            y[rows, cols] = v.astype(BF16)

                    add_rows(n, 6 * g + i, terms, 0, dst, v)

                group(s, g, 8 - n, 1, store)

        return 0

    lax.fori_loop(0, 11, late, 0)

    last = 2
    d2_arrived(8, last)

    def keep(i, v):
        cols = pl.ds(last * V + i * T, T)

        def dst(rows, v):
            accbuf[rows, cols] = v

        add_rows(8, 6 * last + i, terms_0[:2], 0, dst, v)

    group((FINAL + last) % RING, last, 0, 1, keep)
    rs_arrived(7, last)
    for i in range(6):
        cols = pl.ds(last * V + i * T, T)

        def dst(rows, v, cols=cols):
            y[rows, cols] = v.astype(BF16)

        for r in range(0, ROWS, SLICE):
            add_rows(None, 6 * last + i, terms_0[2:], r, dst)

    d2_sent(0)
    d2_sent(1)
    await_bytes(xall.at[:, 0], ag_send.at[0])
    await_bytes(xall.at[pl.ds(0, 4)], ag_send.at[1])
    for s in range(LS):
        sum_sent(s, CH)
    for s in range(3):
        sum_sent(LS + s, V)


def _call(x, wg, wu, wd):
    dma = pltpu.SemaphoreType.DMA
    rows = (ROWS, D)
    return pl.pallas_call(
        _kernel,
        out_shape=(
            pltpu.VMEM(rows, BF16),
            *(pltpu.HBM(shape, BF16) for shape in ((7, 2, *rows), (6, *rows))),
        ),
        in_specs=[pl.BlockSpec(memory_space=pltpu.HBM)] * 4,
        out_specs=[pl.BlockSpec(memory_space=m) for m in (pltpu.VMEM, pltpu.HBM, pltpu.HBM)],
        scratch_shapes=[
            pltpu.VMEM((2, 2 * ROWS, D), BF16),
            pltpu.VMEM((6, *rows), BF16),
            pltpu.VMEM((RING, F, V), BF16),
            pltpu.VMEM(rows, F32),
            pltpu.VMEM((2, ROWS, V), BF16),
            pltpu.VMEM((2, ROWS, T), F32),
            *(dma(s) for s in ((RING,), (3,), (2,), (5,), (2,), (7, 2), (8, 2), (2,), (2, 3), (LS + 3,), (7, 3))),
        ],
        compiler_params=pltpu.CompilerParams(
            collective_id=0, has_side_effects=True, vmem_limit_bytes=64_500_000
        ),
        name="mlp",
    )(x, wg, wu, wd)[0]


def solution(mesh):
    return jax.shard_map(
        _call,
        mesh=mesh,
        in_specs=(P(("dp", "tp"), None), P(None, "tp"), P(None, "tp"), P("tp", None)),
        out_specs=P(("dp", "tp"), None),
        check_vma=False,
    )
```
